32 devices in a mesh: batch: 2 (over x), tp: 4 (over z), sp: 4 (over y, core).
Axes of the slice: x: 2, y: 2, z: 4, core: 2. Of those that a mesh axis runs over, the one named last changes fastest.
Arguments:
- tokens: bfloat16 [16384, 1024], P(('batch', 'sp')), parts along dimension 0
- glob_pos: int32 [1024], P('batch'), parts along dimension 0
- rel_bias: float32 [16, 513], P('tp')
- w_query: bfloat16 [1024, 1024], P(None, 'tp')
- w_key: bfloat16 [1024, 1024], P(None, 'tp')
- w_value: bfloat16 [1024, 1024], P(None, 'tp')
- w_query_glob: bfloat16 [1024, 1024], P(None, 'tp')
- w_out: bfloat16 [1024, 1024], P('tp')
- w_up: bfloat16 [1024, 4096], P(None, 'tp')
- w_down: bfloat16 [4096, 1024], P('tp')
Outputs:
- output: bfloat16 [16384, 1024], P(('batch', 'sp')), parts along dimension 0
There are 2 independent parts. The reference program is written for one: setup_inputs(seed, part) draws one part's arguments, and reference() takes and returns one part's arrays. A program takes and returns all parts, laid end to end along the dimension named above; an argument that names none is the same for every part.
All inputs are finite; a program needn't handle non-finite values.
Results may differ from the reference program's by a relative error of at most 0.0116152.
Values are sent between devices in bfloat16 or wider.
A program may use at most 1 GiB of HBM per device.

```python
import math
import jax
import jax.numpy as jnp
from jax import lax

MODEL_DIM = 1024
NUM_HEADS = 16
HIDDEN_DIM = 4096
WINDOW = 256
NUM_GLOBAL = 512
SEQ_LEN = 8192


def setup_inputs(seed: int = 0, part: int = 0) -> dict:
    part_keys = jax.random.split(jax.random.fold_in(jax.random.key(seed), part), 2)
    shared_keys = jax.random.split(jax.random.key(seed + 1), 9)
    in_scale = MODEL_DIM ** -0.5
    out_scale = ((2 * WINDOW + NUM_GLOBAL) / (3.0 * MODEL_DIM)) ** 0.5
    glob_scale = (math.log(6.0 * SEQ_LEN / (2 * WINDOW + NUM_GLOBAL)) / MODEL_DIM) ** 0.5

    def draw_normal(rand_key, arr_shape, std_dev):
        return (std_dev * jax.random.normal(rand_key, arr_shape, jnp.float32)).astype(jnp.bfloat16)

    square = (MODEL_DIM, MODEL_DIM)
    glob_pos = jnp.sort(jax.random.permutation(part_keys[1], SEQ_LEN)[:NUM_GLOBAL]).astype(jnp.int32)
    return {
        "tokens": draw_normal(part_keys[0], (SEQ_LEN, MODEL_DIM), 1.0),
        "glob_pos": glob_pos,
        "rel_bias": 0.7 * jax.random.normal(shared_keys[0], (NUM_HEADS, 2 * WINDOW + 1), jnp.float32),
        "w_query": draw_normal(shared_keys[1], square, in_scale),
        "w_key": draw_normal(shared_keys[2], square, in_scale),
        "w_value": draw_normal(shared_keys[3], square, in_scale),
        "w_query_glob": draw_normal(shared_keys[4], square, glob_scale),
        "w_out": draw_normal(shared_keys[5], square, out_scale),
        "w_up": draw_normal(shared_keys[6], (MODEL_DIM, HIDDEN_DIM), in_scale),
        "w_down": draw_normal(shared_keys[7], (HIDDEN_DIM, MODEL_DIM), HIDDEN_DIM ** -0.5),
    }


def reference(tokens, glob_pos, rel_bias, w_query, w_key, w_value, w_query_glob, w_out, w_up, w_down):
    head_dim = MODEL_DIM // NUM_HEADS
    score_scale = head_dim ** -0.5
    n_blocks = SEQ_LEN // WINDOW
    heads_shape = (SEQ_LEN, NUM_HEADS, head_dim)

    def project(weight):
        product = jnp.dot(tokens, weight, preferred_element_type=jnp.float32)
        return product.astype(jnp.bfloat16).astype(jnp.float32).reshape(heads_shape)

    queries = project(w_query)
    keys_all = project(w_key)
    values_all = project(w_value)
    zero_pad = jnp.zeros((WINDOW, NUM_HEADS, head_dim), jnp.float32)
    keys_ext = jnp.concatenate([zero_pad, keys_all, zero_pad], axis=0)
    values_ext = jnp.concatenate([zero_pad, values_all, zero_pad], axis=0)
    glob_keys = keys_all[glob_pos]
    glob_values = values_all[glob_pos]
    rel_offs = jnp.arange(3 * WINDOW)[None, :] - jnp.arange(WINDOW)[:, None]
    in_band = (rel_offs >= 0) & (rel_offs <= 2 * WINDOW)
    band_bias = jnp.take(rel_bias, jnp.clip(rel_offs, 0, 2 * WINDOW), axis=1)

    def window_block(blk_index):
        blk_start = blk_index * WINDOW
        q_blk = lax.dynamic_slice_in_dim(queries, blk_start, WINDOW, axis=0)
        k_win = lax.dynamic_slice_in_dim(keys_ext, blk_start, 3 * WINDOW, axis=0)
        v_win = lax.dynamic_slice_in_dim(values_ext, blk_start, 3 * WINDOW, axis=0)
        query_pos = blk_start + jnp.arange(WINDOW)
        key_pos = blk_start - WINDOW + jnp.arange(3 * WINDOW)
        key_ok = (key_pos >= 0) & (key_pos < SEQ_LEN)
        win_scores = jnp.einsum("qhd,khd->hqk", q_blk, k_win) * score_scale + band_bias
        win_scores = jnp.where(in_band & key_ok[None, :], win_scores, -jnp.inf)
        far_mask = jnp.abs(query_pos[:, None] - glob_pos[None, :]) > WINDOW
        glob_scores = jnp.einsum("qhd,ghd->hqg", q_blk, glob_keys) * score_scale
        glob_scores = jnp.where(far_mask, glob_scores, -jnp.inf)
        scores = jnp.concatenate([win_scores, glob_scores], axis=-1)
        attn_probs = jax.nn.softmax(scores, axis=-1).astype(jnp.bfloat16).astype(jnp.float32)
        all_values = jnp.concatenate([v_win, glob_values], axis=0)
        return jnp.einsum("hqk,khd->qhd", attn_probs, all_values)

    win_out = lax.map(window_block, jnp.arange(n_blocks)).reshape(heads_shape)
    x_glob = tokens[glob_pos]
    q_glob = jnp.dot(x_glob, w_query_glob, preferred_element_type=jnp.float32)
    q_glob = q_glob.astype(jnp.bfloat16).astype(jnp.float32).reshape(NUM_GLOBAL // 8, 8, NUM_HEADS, head_dim)

    def glob_block(q_group):
        scores = jnp.einsum("ghd,khd->hgk", q_group, keys_all) * score_scale
        attn_probs = jax.nn.softmax(scores, axis=-1).astype(jnp.bfloat16).astype(jnp.float32)
        return jnp.einsum("hgk,khd->ghd", attn_probs, values_all)

    glob_out = lax.map(glob_block, q_glob).reshape(NUM_GLOBAL, NUM_HEADS, head_dim)
    heads_out = win_out.at[glob_pos].set(glob_out)
    attn_vec = heads_out.reshape(SEQ_LEN, MODEL_DIM).astype(jnp.bfloat16)
    attn_proj = jnp.dot(attn_vec, w_out, preferred_element_type=jnp.float32)
    hidden = (tokens.astype(jnp.float32) + attn_proj).astype(jnp.bfloat16)
    up_proj = jnp.dot(hidden, w_up, preferred_element_type=jnp.float32)
    act_vals = jax.nn.gelu(up_proj).astype(jnp.bfloat16)
    down_proj = jnp.dot(act_vals, w_down, preferred_element_type=jnp.float32)
    return (hidden.astype(jnp.float32) + down_proj).astype(jnp.bfloat16)
```

```python
import functools

import jax
import jax.numpy as jnp
from jax import lax
from jax.experimental import pallas as pl
from jax.experimental.pallas import tpu as pltpu
from jax.sharding import PartitionSpec as P

BLK = 256
F32 = jnp.float32
BF16 = jnp.bfloat16
VMEM_CAP = 60 * 1024 * 1024


def dot_nn(a, b):
    return lax.dot_general(a, b, (((1,), (0,)), ((), ())), preferred_element_type=F32)


def dot_nt(a, b):
    return lax.dot_general(a, b, (((1,), (1,)), ((), ())), preferred_element_type=F32)


def whole(shape):
    return pl.BlockSpec(shape, lambda *_: (0,) * len(shape), pipeline_mode=pl.Buffered(1))


def head_masked(x, head_dim, odd):
    lane = lax.broadcasted_iota(jnp.int32, x.shape, 1)
    keep = (lane >= head_dim) if odd else (lane < head_dim)
    return jnp.where(keep, x, jnp.zeros_like(x))


def project_kernel(scale, slot_ref, x_ref, wq_ref, wk_ref, wv_ref, wg_ref, q_ref, k_ref, v_ref, sel_ref, acc_ref):
    i = pl.program_id(0)
    x = x_ref[...]
    width = wq_ref.shape[1]
    q_ref[...] = dot_nn(x, wq_ref[...]).astype(BF16) * scale
    k = dot_nn(x, wk_ref[...]).astype(BF16)
    v = dot_nn(x, wv_ref[...]).astype(BF16)
    qg = dot_nn(x, wg_ref[...]).astype(BF16) * scale
    k_ref[...] = k
    v_ref[...] = v
    cols = lax.broadcasted_iota(jnp.int32, (slot_ref.shape[0], x.shape[0]), 1) + i * x.shape[0]
    pick = jnp.where(slot_ref[...] == cols, 1.0, 0.0).astype(BF16)

    @pl.when(i == 0)
    def _():
        acc_ref[...] = jnp.zeros_like(acc_ref)

    acc_ref[:, :width] += dot_nn(pick, qg)
    acc_ref[:, width:2 * width] += dot_nn(pick, k)
    acc_ref[:, 2 * width:] += dot_nn(pick, v)

    @pl.when(i == pl.num_programs(0) - 1)
    def _():
        sel_ref[...] = acc_ref[...].astype(BF16)


def project(x, slot_col, wq, wk, wv, wg, scale):
    rows, dim = x.shape
    width = wq.shape[1]
    num_glob = slot_col.shape[0]
    row_block = pl.BlockSpec((BLK, width), lambda i: (i, 0))
    return pl.pallas_call(
        functools.partial(project_kernel, scale),
        grid=(rows // BLK,),
        in_specs=[whole((num_glob, 1)), pl.BlockSpec((BLK, dim), lambda i: (i, 0))] + [whole((dim, width))] * 4,
        out_specs=[row_block, row_block, row_block, pl.BlockSpec((num_glob, 3 * width), lambda i: (0, 0))],
        out_shape=[jax.ShapeDtypeStruct((rows, width), BF16)] * 3 + [jax.ShapeDtypeStruct((num_glob, 3 * width), BF16)],
        scratch_shapes=[pltpu.VMEM((num_glob, 3 * width), F32)],
        compiler_params=pltpu.CompilerParams(vmem_limit_bytes=VMEM_CAP),
        cost_estimate=pl.CostEstimate(flops=2 * rows * dim * width * 4, bytes_accessed=2 * rows * dim * 2, transcendentals=0),
        name="project",
    )(slot_col, x, wq, wk, wv, wg)


def glob_kernel(head_dim, qg_ref, k_ref, v_ref, out_ref, stat_ref):
    k = k_ref[...]
    v = v_ref[...]
    qg = qg_ref[...]
    outs, stats = [], []
    for odd in (False, True):
        s = dot_nt(head_masked(qg, head_dim, odd), k)
        m = jnp.max(s, axis=1, keepdims=True)
        p = jnp.exp(s - m)
        stats.append((m, jnp.sum(p, axis=1, keepdims=True)))
        outs.append(dot_nn(p.astype(BF16), v))
    lane = lax.broadcasted_iota(jnp.int32, out_ref.shape, 1)
    out_ref[...] = jnp.where(lane < head_dim, outs[0], outs[1])
    (m0, l0), (m1, l1) = stats
    stat_ref[...] = jnp.where(lane == 0, m0, jnp.where(lane == 1, m1, jnp.where(lane == 2, l0, l1)))


def glob_partial(sel, k, v, head_dim):
    rows, width = k.shape
    num_glob = sel.shape[0]
    pair = 2 * head_dim
    tile = 128
    kv_spec = pl.BlockSpec((rows, pair), lambda p, i: (0, p))
    out_spec = pl.BlockSpec((tile, pair), lambda p, i: (i, p))
    return pl.pallas_call(
        functools.partial(glob_kernel, head_dim),
        grid=(width // pair, num_glob // tile),
        in_specs=[out_spec, kv_spec, kv_spec],
        out_specs=[out_spec, out_spec],
        out_shape=[jax.ShapeDtypeStruct((num_glob, width), F32)] * 2,
        compiler_params=pltpu.CompilerParams(vmem_limit_bytes=VMEM_CAP),
        cost_estimate=pl.CostEstimate(flops=4 * num_glob * rows * width, bytes_accessed=4 * rows * width, transcendentals=0),
        name="glob_partial",
    )(sel, k, v)


def window_kernel(window, head_dim, blk0, n_blocks, edge_ref, bias_ref, slot_ref, q_ref, kx_ref, vx_ref, sel_ref, gout_ref, o_ref, band_ref):
    step = pl.program_id(0)
    blk = step + blk0
    heads, span = bias_ref.shape[0], bias_ref.shape[2]
    width = 3 * window
    pair = 2 * head_dim
    cols = lax.broadcasted_iota(jnp.int32, (BLK, width), 1)
    cut_left = (blk == 0) & (edge_ref[0] == 1)
    cut_right = (blk == n_blocks - 1) & (edge_ref[1] == 1)

    @pl.when((step == 0) | (blk == 1) | (blk == n_blocks - 1))
    def _():
        lo = jnp.where(cut_left, window, 0)
        hi = jnp.where(cut_right, 2 * window, width)
        for h in range(heads):
            row = jnp.broadcast_to(bias_ref[h], (BLK, span))
            band = pltpu.roll(row, 0, 1, stride=1, stride_axis=0)[:, :width]
            band_ref[h] = jnp.where((cols >= lo) & (cols < hi), band, -jnp.inf)

    slot = slot_ref[...]
    dist = slot - blk * BLK - lax.broadcasted_iota(jnp.int32, (BLK, slot.shape[1]), 0)
    near = jnp.abs(dist) <= window
    pick = jnp.where(dist == 0, 1.0, 0.0)
    is_glob = jnp.max(pick, axis=1, keepdims=True) > 0.0
    pick = pick.astype(BF16)
    start = pl.multiple_of(step * BLK, BLK)
    lane = lax.broadcasted_iota(jnp.int32, (BLK, pair), 1)
    gwidth = gout_ref.shape[1]
    for p in range(heads // 2):
        at = slice(p * pair, (p + 1) * pair)
        q = q_ref[:, at]
        k_win = kx_ref[pl.ds(start, width), at]
        v_win = vx_ref[pl.ds(start, width), at]
        k_glob = sel_ref[:, gwidth + p * pair:gwidth + (p + 1) * pair]
        v_glob = sel_ref[:, 2 * gwidth + p * pair:2 * gwidth + (p + 1) * pair]
        outs = []
        for odd in (False, True):
            qh = head_masked(q, head_dim, odd)
            s_win = dot_nt(qh, k_win) + band_ref[2 * p + int(odd)]
            s_glob = jnp.where(near, -jnp.inf, dot_nt(qh, k_glob))
            m = jnp.maximum(jnp.max(s_win, axis=1, keepdims=True), jnp.max(s_glob, axis=1, keepdims=True))
            e_win = jnp.exp(s_win - m)
            e_glob = jnp.exp(s_glob - m)
            total = jnp.sum(e_win, axis=1, keepdims=True) + jnp.sum(e_glob, axis=1, keepdims=True)
            inv = 1.0 / total
            o = dot_nn((e_win * inv).astype(BF16), v_win)
            outs.append(o + dot_nn((e_glob * inv).astype(BF16), v_glob))
        o = jnp.where(lane < head_dim, outs[0], outs[1])
        ins = dot_nn(pick, gout_ref[:, at])
        o_ref[:, at] = jnp.where(is_glob, ins, o).astype(BF16)


def window_attn(edge, bias, slot_row, q, kx, vx, sel, gout, window, head_dim, chunk, n_chunks):
    rows, width = q.shape
    blocks = rows // BLK
    per = blocks // n_chunks
    num_glob = sel.shape[0]
    heads, _, span = bias.shape
    ext = per * BLK + 2 * window
    kx = lax.slice_in_dim(kx, chunk * per * BLK, chunk * per * BLK + ext)
    vx = lax.slice_in_dim(vx, chunk * per * BLK, chunk * per * BLK + ext)
    return pl.pallas_call(
        functools.partial(window_kernel, window, head_dim, chunk * per, blocks),
        grid=(per,),
        in_specs=[
            pl.BlockSpec(memory_space=pltpu.SMEM),
            whole((heads, 1, span)),
            whole((1, num_glob)),
            pl.BlockSpec((BLK, width), lambda i: (chunk * per + i, 0)),
            whole((ext, width)),
            whole((ext, width)),
            whole((num_glob, 3 * width)),
            whole((num_glob, width)),
        ],
        out_specs=pl.BlockSpec((BLK, width), lambda i: (i, 0)),
        out_shape=jax.ShapeDtypeStruct((per * BLK, width), BF16),
        scratch_shapes=[pltpu.VMEM((heads, BLK, 3 * window), F32)],
        compiler_params=pltpu.CompilerParams(vmem_limit_bytes=VMEM_CAP),
        cost_estimate=pl.CostEstimate(flops=4 * per * BLK * (3 * window + num_glob) * width, bytes_accessed=8 * rows * width, transcendentals=0),
        name="window_attn",
    )(edge, bias, slot_row, q, kx, vx, sel, gout)


def mlp_kernel(n_tp, o_ref, x_ref, wo_ref, wu_ref, wd_ref, out_ref):
    dim = x_ref.shape[1]
    shard = o_ref.shape[2]
    acc = x_ref[...].astype(F32)
    for t in range(n_tp):
        acc += dot_nn(o_ref[t], wo_ref[:, t].reshape(shard, dim))
    hidden = acc.astype(BF16)
    acc = hidden.astype(F32)
    for t in range(n_tp):
        up = dot_nn(hidden, wu_ref[:, t].reshape(dim, -1))
        act = jax.nn.gelu(up).astype(BF16)
        acc += dot_nn(act, wd_ref[:, t].reshape(-1, dim))
    out_ref[...] = acc.astype(BF16)


def mlp(o_all, x, packed, chunk):
    n_tp, rows, shard = o_all.shape
    dim = x.shape[1]
    nb, _, ns, _, _ = packed.shape
    up_rows = dim // (nb * ns)
    out_rows = shard // (nb * ns)
    tile = 256
    first = chunk * (rows // tile)
    big = (nb, n_tp, ns, up_rows, dim)
    return pl.pallas_call(
        functools.partial(mlp_kernel, n_tp),
        grid=(rows // tile,),
        in_specs=[
            pl.BlockSpec((n_tp, tile, shard), lambda i: (0, i, 0)),
            pl.BlockSpec((tile, dim), lambda i: (first + i, 0)),
            pl.BlockSpec((nb, n_tp, ns, out_rows, dim), lambda i: (0, 0, 0, 2 * up_rows // out_rows, 0), pipeline_mode=pl.Buffered(1)),
            pl.BlockSpec(big, lambda i: (0, 0, 0, 0, 0), pipeline_mode=pl.Buffered(1)),
            pl.BlockSpec(big, lambda i: (0, 0, 0, 1, 0), pipeline_mode=pl.Buffered(1)),
        ],
        out_specs=pl.BlockSpec((tile, dim), lambda i: (i, 0)),
        out_shape=jax.ShapeDtypeStruct((rows, dim), BF16),
        compiler_params=pltpu.CompilerParams(vmem_limit_bytes=VMEM_CAP),
        cost_estimate=pl.CostEstimate(flops=2 * rows * dim * dim * 9, bytes_accessed=4 * rows * dim, transcendentals=0),
        name="mlp",
    )(o_all, x, packed, packed, packed)


def solution(mesh):
    n_seq = mesh.shape["sp"]
    n_tp = mesh.shape["tp"]
    n_batch = mesh.shape["batch"]
    to_right = [(sender, sender + 1) for sender in range(n_seq - 1)]
    to_left = [(sender + 1, sender) for sender in range(n_seq - 1)]

    def local_layer(tokens, glob_pos, rel_bias, w_query, w_key, w_value, w_query_glob, w_out, w_up, w_down):
        rows, dim = tokens.shape
        heads = rel_bias.shape[0]
        window = (rel_bias.shape[1] - 1) // 2
        width = w_query.shape[1]
        head_dim = width // heads
        num_glob = glob_pos.shape[0]
        sp = lax.axis_index("sp")
        slot = glob_pos - sp * rows

        replica = lax.axis_index("batch") * n_seq + sp
        n_rep = n_batch * n_seq

        def my_rows(weight):
            size = weight.shape[0] // n_rep
            return lax.dynamic_slice_in_dim(weight, replica * size, size)

        piece = jnp.concatenate([my_rows(w_up), my_rows(w_down), my_rows(w_out)])
        packed = lax.all_gather(piece, ("batch", "tp", "sp"), axis=0, tiled=False)
        packed = packed.reshape(n_batch, n_tp, n_seq, *piece.shape)

        q, k, v, sel = project(tokens, slot[:, None], w_query, w_key, w_value, w_query_glob, head_dim ** -0.5)

        def spread(part):
            return lax.all_to_all(part, "sp", 0, 0)

        share = num_glob // n_seq
        got = spread(sel.reshape(n_seq, share, 3 * width))
        mine = got.astype(F32).sum(axis=0).astype(BF16)
        sel = spread(jnp.broadcast_to(mine[None], (n_seq,) + mine.shape)).reshape(num_glob, 3 * width)

        kv = jnp.stack([k, v])
        left = lax.ppermute(kv[:, rows - window:], "sp", to_right)
        right = lax.ppermute(kv[:, :window], "sp", to_left)
        kx = jnp.concatenate([left[0], k, right[0]])
        vx = jnp.concatenate([left[1], v, right[1]])

        part_out, part_stat = glob_partial(sel, k, v, head_dim)
        got_out = spread(part_out.reshape(n_seq, share, width))
        stat = part_stat.reshape(num_glob, heads // 2, 2 * head_dim)[:, :, :4]
        got_stat = spread(stat.reshape(n_seq, share, heads // 2, 2, 2))
        part_max = got_stat[:, :, :, 0].reshape(n_seq, share, heads)
        part_sum = got_stat[:, :, :, 1].reshape(n_seq, share, heads)
        rescale = jnp.exp(part_max - part_max.max(axis=0))
        inv = 1.0 / (part_sum * rescale).sum(axis=0)
        merged = (got_out.reshape(n_seq, share, heads, head_dim) * rescale[..., None]).sum(axis=0) * inv[..., None]
        merged = merged.astype(BF16).reshape(share, width)
        gout = spread(jnp.broadcast_to(merged[None], (n_seq,) + merged.shape)).reshape(num_glob, width)

        span = 4 * window
        bias = jnp.pad(rel_bias, ((0, 0), (0, span - rel_bias.shape[1])), constant_values=-jnp.inf)[:, None]
        edge = jnp.stack([sp == 0, sp == n_seq - 1]).astype(jnp.int32)
        n_chunks = 4
        outs = []
        for c in range(n_chunks):
            o = window_attn(edge, bias, slot[None], q, kx, vx, sel, gout, window, head_dim, c, n_chunks)
            o_all = lax.all_gather(o, "tp", axis=0)
            outs.append(mlp(o_all, tokens, packed, c))
        return jnp.concatenate(outs)

    row_spec = P(("batch", "sp"), None)
    col_spec = P(None, "tp")
    head_spec = P("tp", None)
    in_specs = (row_spec, P("batch"), head_spec, col_spec, col_spec, col_spec, col_spec, head_spec, col_spec, head_spec)
    return jax.shard_map(local_layer, mesh=mesh, in_specs=in_specs, out_specs=row_spec, check_vma=False)
```

```python
import functools

import jax
import jax.numpy as jnp
from jax import lax
from jax.experimental import pallas as pl
from jax.experimental.pallas import tpu as pltpu
from jax.sharding import PartitionSpec as P

BLK = 256
F32 = jnp.float32
BF16 = jnp.bfloat16
MESH = pl.DeviceIdType.MESH
VMEM_CAP = 67043328


def dot_nn(a, b):
    return lax.dot_general(a, b, (((1,), (0,)), ((), ())), preferred_element_type=F32)


def dot_nt(a, b):
    return lax.dot_general(a, b, (((1,), (1,)), ((), ())), preferred_element_type=F32)


def layer_kernel(
    n_tp, n_seq, window, head_dim, heads,
    slot_col, slot_row, bias_ref, x_hbm, wq_hbm, wk_hbm, wv_hbm, wg_hbm, wu_hbm, wd_hbm, wo_hbm,
    out_hbm,
    x_ref, wq_ref, wk_ref, wv_ref, wg_ref, wbuf, q_ref, kvx, acc_ref, sel_ref, sel_r1, sel_s1, sel_r2, sel_all,
    band_ref, g_ref, g_r1, g_s1, g_r2, gout_ref, o_raw, o_all, stage,
    x_sem, w_sem, own_sem, out_sem, halo_s, halo_r, sel_s, sel_r, g_s, g_r,
    z_s, z_r, zr_s, a_s, a_r, b_s, b_r, c_s, c_r, o_s, o_r, or_s,
):
    rows, dim = x_ref.shape
    width = wq_ref.shape[1]
    num_glob = slot_col.shape[0]
    half = num_glob // 2
    blocks = rows // BLK
    span = bias_ref.shape[2]
    band_w = 3 * window
    pair = 2 * head_dim
    scale = head_dim ** -0.5
    up_rows = wu_hbm.shape[1]
    out_rows = wo_hbm.shape[1]
    piece_rows = 2 * up_rows + out_rows
    cut = piece_rows // 2

    b = lax.axis_index("batch")
    t = lax.axis_index("tp")
    s = lax.axis_index("sp")
    core = s % 2
    partner = {"sp": s + 1 - 2 * core}
    y_peer = {"sp": (s + 2) % 4}
    x_peer = {"batch": 1 - b}
    near = t + 1 - 2 * (t % 2)
    side = t // 2
    across = 2 - side
    far = 3 - 3 * side
    inner = (t == 1) | (t == 2)
    near_dev, across_dev = {"tp": near}, {"tp": across}
    srcs = (near, across, far)
    rep = b * n_seq + s
    rep_x = (1 - b) * n_seq + s
    rep_y = b * n_seq + (s + 2) % 4
    rep_d = (1 - b) * n_seq + (s + 2) % 4

    def remote(src, dst, ssem, rsem, dev):
        return pltpu.make_async_remote_copy(src_ref=src, dst_ref=dst, send_sem=ssem, recv_sem=rsem, device_id=dev, device_id_type=MESH)

    def load_x(i):
        at = pl.ds(pl.multiple_of(i * BLK, BLK), BLK)
        return pltpu.make_async_copy(x_hbm.at[at], x_ref.at[at], x_sem.at[i])

    own = [
        pltpu.make_async_copy(wu_hbm, wbuf.at[t, :, pl.ds(0, up_rows)], own_sem.at[0]),
        pltpu.make_async_copy(wd_hbm, wbuf.at[t, :, pl.ds(up_rows, up_rows)], own_sem.at[1]),
        pltpu.make_async_copy(wo_hbm, wbuf.at[t, :, pl.ds(2 * up_rows, out_rows)], own_sem.at[2]),
    ]
    wload = [pltpu.make_async_copy(h, v, w_sem.at[j]) for j, (h, v) in enumerate(((wk_hbm, wk_ref), (wv_hbm, wv_ref), (wg_hbm, wg_ref), (wq_hbm, wq_ref)))]
    for copy in own:
        copy.start()
    for copy in wload:
        copy.start()
    for i in range(blocks):
        load_x(i).start()

    barrier = pltpu.get_barrier_semaphore()
    peers = [{"tp": (t + d) % n_tp} for d in (1, 2, 3)] + [{"sp": (s + d) % n_seq} for d in (1, 2, 3)] + [x_peer]
    for dev in peers:
        pl.semaphore_signal(barrier, inc=1, device_id=dev, device_id_type=MESH)
    pl.semaphore_wait(barrier, len(peers))
    for copy in own:
        copy.wait()

    def piece(src, r):
        return wbuf.at[src, r]

    def z_copy(j):
        return remote(piece(t, rep), piece(t, rep), z_s.at[j], z_r.at[t], (near_dev, across_dev)[j])

    def z_wait(k):
        remote(piece(srcs[k], rep), piece(srcs[k], rep), z_s.at[0], z_r.at[srcs[k]], near_dev).wait_recv()

    def z_relay(k):
        return remote(piece(srcs[k], rep), piece(srcs[k], rep), zr_s.at[k - 1], z_r.at[srcs[k]], near_dev)

    def a_copy(k, j):
        return remote(piece(srcs[k], rep), piece(srcs[k], rep), a_s.at[k, j], a_r.at[k, j], (x_peer, y_peer, partner)[j])

    def a_wait(k, j):
        r = (rep_x, rep_y)[j]
        remote(piece(srcs[k], r), piece(srcs[k], r), a_s.at[k, j], a_r.at[k, j], (x_peer, y_peer)[j]).wait_recv()

    def b_copy(k, j):
        r = (rep_x, rep_y, rep_x, rep_y)[j]
        ref = piece(srcs[k], r)
        if j == 2:
            ref = wbuf.at[srcs[k], r, pl.ds(0, cut)]
        if j == 3:
            ref = wbuf.at[srcs[k], r, pl.ds(cut, cut)]
        return remote(ref, ref, b_s.at[k, j], b_r.at[k, j], (partner, partner, y_peer, x_peer)[j])

    def b_wait(k, j):
        ref = wbuf.at[srcs[k], rep_d, pl.ds(0 if j == 2 else cut, cut)]
        remote(ref, ref, b_s.at[k, j], b_r.at[k, j], partner).wait_recv()

    def c_copy(k):
        return remote(piece(srcs[k], rep_d), piece(srcs[k], rep_d), c_s.at[k], c_r.at[k], partner)

    def phase_a(k):
        for j in range(3):
            a_copy(k, j).start()

    def phase_b(k):
        a_wait(k, 0)
        b_copy(k, 2).start()
        b_copy(k, 0).start()
        a_wait(k, 1)
        b_copy(k, 3).start()
        b_copy(k, 1).start()

    def phase_c(k):
        b_wait(k, 2)
        b_wait(k, 3)
        c_copy(k).start()

    def weights_done():
        rp = (s + 1 - 2 * core)
        base, basex = b * n_seq, (1 - b) * n_seq
        for k in range(3):
            remote(piece(srcs[k], base + rp), piece(srcs[k], base + rp), a_s.at[k, 2], a_r.at[k, 2], partner).wait_recv()
            remote(piece(srcs[k], basex + rp), piece(srcs[k], basex + rp), b_s.at[k, 0], b_r.at[k, 0], partner).wait_recv()
            ry = (rp + 2) % 4
            remote(piece(srcs[k], base + ry), piece(srcs[k], base + ry), b_s.at[k, 1], b_r.at[k, 1], partner).wait_recv()
            remote(piece(srcs[k], basex + ry), piece(srcs[k], basex + ry), c_s.at[k], c_r.at[k], partner).wait_recv()

    z_copy(0).start()
    z_copy(1).start()

    acc_ref[...] = jnp.zeros_like(acc_ref)
    for copy in wload[:3]:
        copy.wait()

    def project(i, carry):
        load_x(i).wait()
        at = pl.ds(pl.multiple_of(i * BLK, BLK), BLK)
        x = x_ref[at, :]
        k = dot_nn(x, wk_ref[...]).astype(BF16)
        v = dot_nn(x, wv_ref[...]).astype(BF16)
        qg = dot_nn(x, wg_ref[...]).astype(BF16) * scale
        ext = pl.ds(pl.multiple_of(i * BLK + window, BLK), BLK)
        kvx[ext, :width] = k
        kvx[ext, width:] = v
        cols = lax.broadcasted_iota(jnp.int32, (num_glob, BLK), 1) + i * BLK
        pick = jnp.where(slot_col[...] == cols, 1.0, 0.0).astype(BF16)
        acc_ref[:, :width] += dot_nn(pick, qg)
        acc_ref[:, width:2 * width] += dot_nn(pick, k)
        acc_ref[:, 2 * width:] += dot_nn(pick, v)
        return carry

    lax.fori_loop(0, blocks, project, 0)
    sel_ref[...] = acc_ref[...].astype(BF16)

    mine = pl.ds(pl.multiple_of(core * half, half), half)
    theirs = pl.ds(pl.multiple_of((1 - core) * half, half), half)

    def swap(ref, r1, s1, r2, full, ssem, rsem):
        first = remote(ref.at[theirs], r1, ssem.at[0], rsem.at[0], partner)
        second = remote(s1, r2, ssem.at[1], rsem.at[1], y_peer)
        third = remote(full.at[mine], full.at[mine], ssem.at[2], rsem.at[2], partner)
        third_in = remote(full.at[theirs], full.at[theirs], ssem.at[2], rsem.at[2], partner)
        return first, second, third, third_in

    sel1, sel2, sel3, sel3_in = swap(sel_ref, sel_r1, sel_s1, sel_r2, sel_all, sel_s, sel_r)
    sel1.start()
    edge = (pl.ds(window, window), pl.ds(rows, window))
    halo_left = remote(kvx.at[edge[0]], kvx.at[pl.ds(rows + window, window)], halo_s.at[0], halo_r.at[0], {"sp": (s + 3) % n_seq})
    halo_right = remote(kvx.at[edge[1]], kvx.at[pl.ds(0, window)], halo_s.at[1], halo_r.at[1], {"sp": (s + 1) % n_seq})
    sel1.wait_recv()
    sel_s1[...] = sel_ref[mine, :] + sel_r1[...]
    sel2.start()
    halo_left.start()
    halo_right.start()

    z_wait(0)
    phase_a(0)

    @pl.when(inner)
    def _():
        z_wait(1)
        z_relay(1).start()

    wload[3].wait()

    def project_q(i, carry):
        at = pl.ds(pl.multiple_of(i * BLK, BLK), BLK)
        q_ref[at, :] = dot_nn(x_ref[at, :], wq_ref[...]).astype(BF16) * scale
        return carry

    lax.fori_loop(0, blocks, project_q, 0)

    cols = lax.broadcasted_iota(jnp.int32, (BLK, band_w), 1)

    def make_band(lo, hi):
        for h in range(heads):
            row = jnp.broadcast_to(bias_ref[h], (BLK, span))
            band = pltpu.roll(row, 0, 1, stride=1, stride_axis=0)[:, :band_w]
            band_ref[h] = jnp.where((cols >= lo) & (cols < hi), band, -jnp.inf)

    is_first = 1 - (s + n_seq - 1) // n_seq
    is_last = s // (n_seq - 1)
    make_band(window * is_first, band_w)

    sel2.wait_recv()
    sel_all[mine, :] = sel_s1[...] + sel_r2[...]
    sel3.start()

    @pl.when(jnp.logical_not(inner))
    def _():
        z_wait(1)

    phase_a(1)

    @pl.when(inner)
    def _():
        z_wait(2)
        z_relay(2).start()

    sel3_in.wait_recv()

    lane_p = lax.broadcasted_iota(jnp.int32, (1, pair), 1)
    low = lane_p < head_dim
    zero = jnp.zeros((), BF16)
    tile = 128

    def masked(xv, odd):
        return jnp.where(low, zero, xv) if odd else jnp.where(low, xv, zero)

    def glob(i, carry):
        at = pl.ds(pl.multiple_of(i * tile, tile), tile)
        lane = lax.broadcasted_iota(jnp.int32, (tile, 128), 1)
        stat = jnp.zeros((tile, 128), F32)
        for p in range(heads // 2):
            qg = sel_all[at, p * pair:(p + 1) * pair]
            k = kvx[pl.ds(window, rows), p * pair:(p + 1) * pair]
            v = kvx[pl.ds(window, rows), width + p * pair:width + (p + 1) * pair]
            outs = []
            for odd in (0, 1):
                sc = dot_nt(masked(qg, odd), k)
                m = jnp.max(sc, axis=1, keepdims=True)
                e = jnp.exp(sc - m)
                stat = jnp.where(lane == 2 * p + odd, m, stat)
                stat = jnp.where(lane == heads + 2 * p + odd, jnp.sum(e, axis=1, keepdims=True), stat)
                outs.append(dot_nn(e.astype(BF16), v))
            g_ref[at, p * pair:(p + 1) * pair] = jnp.where(low, outs[0], outs[1])
        g_ref[at, width:] = stat
        return carry

    lax.fori_loop(0, num_glob // tile, glob, 0)

    def merge(a, c):
        sa, sc = a[:, width:], c[:, width:]
        lane = lax.broadcasted_iota(jnp.int32, sa.shape, 1)
        wide = lax.broadcasted_iota(jnp.int32, (1, width), 1)
        fa = jnp.zeros((sa.shape[0], width), F32)
        fc, total = fa, fa
        stat = jnp.zeros_like(sa)
        for h in range(heads):
            ma, mc = sa[:, h:h + 1], sc[:, h:h + 1]
            la, lc = sa[:, heads + h:heads + h + 1], sc[:, heads + h:heads + h + 1]
            m = jnp.maximum(ma, mc)
            ea, ec = jnp.exp(ma - m), jnp.exp(mc - m)
            l = la * ea + lc * ec
            here = (wide >= h * head_dim) & (wide < (h + 1) * head_dim)
            fa = jnp.where(here, ea, fa)
            fc = jnp.where(here, ec, fc)
            total = jnp.where(here, l, total)
            stat = jnp.where(lane == h, m, stat)
            stat = jnp.where(lane == heads + h, l, stat)
        return a[:, :width] * fa + c[:, :width] * fc, total, stat

    g1, g2, g3, g3_in = swap(g_ref, g_r1, g_s1, g_r2, gout_ref, g_s, g_r)
    g1.start()
    halo_left.wait_recv()
    halo_right.wait_recv()

    slot = slot_row[...]
    lane_b = lax.broadcasted_iota(jnp.int32, (BLK, pair), 1)
    row_iota = lax.broadcasted_iota(jnp.int32, (BLK, num_glob), 0)

    def attend(i):
        dist = slot - i * BLK - row_iota
        near_by = jnp.abs(dist) <= window
        start = pl.multiple_of(i * BLK, BLK)
        for p in range(heads // 2):
            at = slice(p * pair, (p + 1) * pair)
            q = q_ref[pl.ds(start, BLK), at]
            k_win = kvx[pl.ds(start, band_w), at]
            v_win = kvx[pl.ds(start, band_w), width + p * pair:width + (p + 1) * pair]
            k_glob = sel_all[:, width + p * pair:width + (p + 1) * pair]
            v_glob = sel_all[:, 2 * width + p * pair:2 * width + (p + 1) * pair]
            outs = []
            for odd in (0, 1):
                qh = masked(q, odd)
                s_win = dot_nt(qh, k_win) + band_ref[2 * p + odd]
                s_glob = jnp.where(near_by, -jnp.inf, dot_nt(qh, k_glob))
                m = jnp.maximum(jnp.max(s_win, axis=1, keepdims=True), jnp.max(s_glob, axis=1, keepdims=True))
                e_win = jnp.exp(s_win - m)
                e_glob = jnp.exp(s_glob - m)
                inv = 1.0 / (jnp.sum(e_win, axis=1, keepdims=True) + jnp.sum(e_glob, axis=1, keepdims=True))
                o = dot_nn((e_win * inv).astype(BF16), v_win)
                outs.append(o + dot_nn((e_glob * inv).astype(BF16), v_glob))
            o_raw[pl.ds(start, BLK), at] = jnp.where(low, outs[0], outs[1]).astype(BF16)

    def block_ref(src, j):
        return o_all.at[src, pl.ds(pl.multiple_of(j * BLK, BLK), BLK)]

    def o_copy(j, way):
        return remote(block_ref(t, j), block_ref(t, j), o_s.at[way, j], o_r.at[t, j], (near_dev, across_dev)[way])

    def o_wait(src, j):
        remote(block_ref(src, j), block_ref(src, j), o_s.at[0, 0], o_r.at[src, j], near_dev).wait_recv()

    def o_relay(k, j):
        return remote(block_ref(srcs[k], j), block_ref(srcs[k], j), or_s.at[k - 1, j], o_r.at[srcs[k], j], near_dev)

    def finish(j, carry):
        at = pl.ds(pl.multiple_of(j * BLK, BLK), BLK)
        pick = jnp.where(slot - j * BLK == row_iota, 1.0, 0.0)
        is_glob = jnp.max(pick, axis=1, keepdims=True) > 0.0
        ins = dot_nn(pick.astype(BF16), gout_ref[...])
        o_all[t, at, :] = jnp.where(is_glob, ins, o_raw[at, :].astype(F32)).astype(BF16)
        o_copy(j, 0).start()
        o_copy(j, 1).start()
        return carry

    def relay(j, carry):
        for k in (1, 2):
            o_wait(srcs[k], j)
            o_relay(k, j).start()
        return carry

    def relays(lo, hi):
        @pl.when(inner)
        def _():
            lax.fori_loop(lo, hi, relay, 0)

    lag = 3

    def window_step(i, carry):
        attend(i)

        @pl.when(i == 0)
        def _():
            make_band(0, band_w)
            g1.wait_recv()
            num, total, stat = merge(g_ref[mine, :], g_r1[...])
            g_s1[:, :width] = num
            g_s1[:, width:] = stat
            g2.start()

            @pl.when(jnp.logical_not(inner))
            def _():
                z_wait(2)

            phase_b(0)
            phase_a(2)

        @pl.when(i == 2)
        def _():
            g2.wait_recv()
            num, total, stat = merge(g_s1[...], g_r2[...])
            gout_ref[mine, :] = (num / total).astype(BF16)
            g3.start()
            phase_b(1)

        @pl.when(i == 4)
        def _():
            phase_b(2)
            phase_c(0)

        @pl.when(i == 6)
        def _():
            make_band(0, band_w - window * is_last)
            phase_c(1)

        @pl.when(i == lag)
        def _():
            g3_in.wait_recv()
            lax.fori_loop(0, lag, finish, 0)

        @pl.when(i >= lag)
        def _():
            finish(i, 0)

        @pl.when(i == 5)
        def _():
            relays(0, 1)

        @pl.when(i == 6)
        def _():
            relays(1, 2)

        @pl.when(i == 7)
        def _():
            relays(2, 4)

        return carry

    lax.fori_loop(0, blocks, window_step, 0)
    phase_c(2)
    weights_done()

    def out_copy(i):
        return pltpu.make_async_copy(stage.at[i % 2], out_hbm.at[pl.ds(pl.multiple_of(i * BLK, BLK), BLK)], out_sem.at[i % 2])

    def mlp(i, carry):
        at = pl.ds(pl.multiple_of(i * BLK, BLK), BLK)
        o_wait(near, i)

        @pl.when(jnp.logical_not(inner))
        def _():
            o_wait(across, i)
            o_wait(far, i)

        acc = x_ref[at, :].astype(F32)
        for j in range(n_tp):
            acc += dot_nn(o_all[j, at, :], wbuf[j, :, 2 * up_rows:, :].reshape(width, dim))
        hidden = acc.astype(BF16)
        acc = hidden.astype(F32)
        for j in range(n_tp):
            up = dot_nn(hidden, wbuf[j, :, :up_rows, :].reshape(dim, dim))
            acc += dot_nn(jax.nn.gelu(up).astype(BF16), wbuf[j, :, up_rows:2 * up_rows, :].reshape(dim, dim))

        @pl.when(i >= 2)
        def _():
            out_copy(i - 2).wait()

        stage[i % 2] = acc.astype(BF16)
        out_copy(i).start()

        @pl.when(i == 0)
        def _():
            relays(4, 6)

        @pl.when(i == 1)
        def _():
            relays(6, 7)

        @pl.when(i == 2)
        def _():
            relays(7, 8)

        return carry

    lax.fori_loop(0, blocks, mlp, 0)

    out_copy(blocks - 2).wait()
    out_copy(blocks - 1).wait()
    for copy in (halo_left, halo_right, sel1, sel2, sel3, g1, g2, g3, z_copy(0), z_copy(1)):
        copy.wait_send()
    for k in range(3):
        for j in range(3):
            a_copy(k, j).wait_send()
        for j in range(4):
            b_copy(k, j).wait_send()
        c_copy(k).wait_send()

    def drain(j, carry):
        o_copy(j, 0).wait_send()
        o_copy(j, 1).wait_send()
        return carry

    lax.fori_loop(0, blocks, drain, 0)

    @pl.when(inner)
    def _():
        z_relay(1).wait_send()
        z_relay(2).wait_send()

        def drain_relay(j, carry):
            o_relay(1, j).wait_send()
            o_relay(2, j).wait_send()
            return carry

        lax.fori_loop(0, blocks, drain_relay, 0)


def solution(mesh):
    n_seq = mesh.shape["sp"]
    n_tp = mesh.shape["tp"]
    n_batch = mesh.shape["batch"]
    n_rep = n_seq * n_batch

    def local_layer(tokens, glob_pos, rel_bias, w_query, w_key, w_value, w_query_glob, w_out, w_up, w_down):
        rows, dim = tokens.shape
        heads = rel_bias.shape[0]
        window = (rel_bias.shape[1] - 1) // 2
        width = w_query.shape[1]
        head_dim = width // heads
        num_glob = glob_pos.shape[0]
        half = num_glob // 2
        slot = glob_pos - lax.axis_index("sp") * rows
        span = 4 * window
        bias = jnp.pad(rel_bias, ((0, 0), (0, span - rel_bias.shape[1])), constant_values=-jnp.inf)[:, None]
        blocks = rows // BLK
        up_rows, out_rows = dim // n_rep, width // n_rep
        stat_w = width + 128
        any_spec = pl.BlockSpec(memory_space=pl.ANY)
        vmem_spec = pl.BlockSpec(memory_space=pltpu.VMEM)
        dma = pltpu.SemaphoreType.DMA
        return pl.pallas_call(
            functools.partial(layer_kernel, n_tp, n_seq, window, head_dim, heads),
            out_shape=jax.ShapeDtypeStruct((rows, dim), BF16),
            in_specs=[vmem_spec] * 3 + [any_spec] * 8,
            out_specs=any_spec,
            scratch_shapes=[
                pltpu.VMEM((rows, dim), BF16),
                pltpu.VMEM((dim, width), BF16),
                pltpu.VMEM((dim, width), BF16),
                pltpu.VMEM((dim, width), BF16),
                pltpu.VMEM((dim, width), BF16),
                pltpu.VMEM((n_tp, n_rep, 2 * up_rows + out_rows, dim), BF16),
                pltpu.VMEM((rows, width), BF16),
                pltpu.VMEM((rows + 2 * window, 2 * width), BF16),
                pltpu.VMEM((num_glob, 3 * width), F32),
                pltpu.VMEM((num_glob, 3 * width), BF16),
                pltpu.VMEM((half, 3 * width), BF16),
                pltpu.VMEM((half, 3 * width), BF16),
                pltpu.VMEM((half, 3 * width), BF16),
                pltpu.VMEM((num_glob, 3 * width), BF16),
                pltpu.VMEM((heads, BLK, 3 * window), F32),
                pltpu.VMEM((num_glob, stat_w), F32),
                pltpu.VMEM((half, stat_w), F32),
                pltpu.VMEM((half, stat_w), F32),
                pltpu.VMEM((half, stat_w), F32),
                pltpu.VMEM((num_glob, width), BF16),
                pltpu.VMEM((rows, width), BF16),
                pltpu.VMEM((n_tp, rows, width), BF16),
                pltpu.VMEM((2, BLK, dim), BF16),
                dma((blocks,)), dma((4,)), dma((3,)), dma((2,)),
                dma((2,)), dma((2,)), dma((3,)), dma((3,)), dma((3,)), dma((3,)),
                dma((2,)), dma((n_tp,)), dma((2,)),
                dma((3, 3)), dma((3, 3)), dma((3, 4)), dma((3, 4)), dma((3,)), dma((3,)),
                dma((2, blocks)), dma((n_tp, blocks)), dma((2, blocks)),
            ],
            compiler_params=pltpu.CompilerParams(vmem_limit_bytes=VMEM_CAP, collective_id=0, has_side_effects=True),
            name="layer",
        )(
            slot[:, None], slot[None], bias, tokens, w_query, w_key, w_value, w_query_glob,
            w_up.reshape(n_rep, up_rows, dim), w_down.reshape(n_rep, up_rows, dim), w_out.reshape(n_rep, out_rows, dim),
        )

    row_spec = P(("batch", "sp"), None)
    col_spec = P(None, "tp")
    head_spec = P("tp", None)
    in_specs = (row_spec, P("batch"), head_spec, col_spec, col_spec, col_spec, col_spec, head_spec, col_spec, head_spec)
    return jax.shard_map(local_layer, mesh=mesh, in_specs=in_specs, out_specs=row_spec, check_vma=False)
```

```python
import functools

import jax
import jax.numpy as jnp
from jax import lax
from jax.experimental import pallas as pl
from jax.experimental.pallas import tpu as pltpu
from jax.sharding import PartitionSpec as P

BLK = 256
F32 = jnp.float32
BF16 = jnp.bfloat16
MESH = pl.DeviceIdType.MESH
VMEM_CAP = 67043328


def dot_nn(a, b):
    return lax.dot_general(a, b, (((1,), (0,)), ((), ())), preferred_element_type=F32)


def dot_nt(a, b):
    return lax.dot_general(a, b, (((1,), (1,)), ((), ())), preferred_element_type=F32)


def layer_kernel(
    n_tp, n_seq, window, head_dim, heads,
    slot_col, slot_row, bias_ref, x_hbm, wq_hbm, wk_hbm, wv_hbm, wg_hbm, wu_hbm, wd_hbm, wo_hbm,
    out_hbm,
    x_ref, wq_ref, wk_ref, wv_ref, wg_ref, wbuf, q_ref, kvx, acc_ref, qsel_ref, qsel_r1, qsel_s1, qsel_r2, qsel_all, sel_ref, sel_r1, sel_s1, sel_r2, sel_all,
    band_ref, g_ref, g_r1, g_s1, g_r2, gout_ref, o_raw, o_all, stage,
    x_sem, w_sem, own_sem, out_sem, halo_s, halo_r, qsel_s, qsel_r, sel_s, sel_r, g_s, g_r,
    z_s, z_r, zr_s, a_s, a_r, b_s, b_r, c_s, c_r, o_s, o_r, or_s,
):
    rows, dim = x_ref.shape
    width = wq_ref.shape[1]
    num_glob = slot_col.shape[0]
    half = num_glob // 2
    blocks = rows // BLK
    span = bias_ref.shape[2]
    band_w = 3 * window
    pair = 2 * head_dim
    scale = head_dim ** -0.5
    up_rows = wu_hbm.shape[1]
    out_rows = wo_hbm.shape[1]
    part_rows = (2 * up_rows + out_rows) // 2
    cut = part_rows // 3

    b = lax.axis_index("batch")
    t = lax.axis_index("tp")
    s = lax.axis_index("sp")
    core = s % 2
    partner = {"sp": s + 1 - 2 * core}
    y_peer = {"sp": (s + 2) % 4}
    x_peer = {"batch": 1 - b}
    near = t + 1 - 2 * (t % 2)
    side = t // 2
    across = 2 - side
    far = 3 - 3 * side
    inner = (t == 1) | (t == 2)
    near_dev, across_dev = {"tp": near}, {"tp": across}
    srcs = (near, across, far)
    rep = b * n_seq + s
    rep_x = (1 - b) * n_seq + s
    rep_y = b * n_seq + (s + 2) % 4
    rep_d = (1 - b) * n_seq + (s + 2) % 4

    def remote(src, dst, ssem, rsem, dev):
        return pltpu.make_async_remote_copy(src_ref=src, dst_ref=dst, send_sem=ssem, recv_sem=rsem, device_id=dev, device_id_type=MESH)

    def load_x(i):
        at = pl.ds(pl.multiple_of(i * BLK, BLK), BLK)
        return pltpu.make_async_copy(x_hbm.at[at], x_ref.at[at], x_sem.at[i])

    own = [
        pltpu.make_async_copy(wu_hbm, wbuf.at[t, :, pl.ds(0, up_rows)], own_sem.at[0]),
        pltpu.make_async_copy(wd_hbm, wbuf.at[t, :, pl.ds(up_rows, up_rows)], own_sem.at[1]),
        pltpu.make_async_copy(wo_hbm, wbuf.at[t, :, pl.ds(2 * up_rows, out_rows)], own_sem.at[2]),
    ]
    wload = [pltpu.make_async_copy(h, v, w_sem.at[j]) for j, (h, v) in enumerate(((wk_hbm, wk_ref), (wv_hbm, wv_ref), (wg_hbm, wg_ref), (wq_hbm, wq_ref)))]
    for copy in own:
        copy.start()
    for copy in wload:
        copy.start()
    for i in range(blocks):
        load_x(i).start()

    barrier = pltpu.get_barrier_semaphore()
    peers = [{"tp": (t + d) % n_tp} for d in (1, 2, 3)] + [{"sp": (s + d) % n_seq} for d in (1, 2, 3)] + [x_peer]
    for dev in peers:
        pl.semaphore_signal(barrier, inc=1, device_id=dev, device_id_type=MESH)
    pl.semaphore_wait(barrier, len(peers))
    for copy in own:
        copy.wait()

    def piece(src, r, c, lo=0, size=part_rows):
        return wbuf.at[src, r, pl.ds(c * part_rows + lo, size)]

    def z_copy(j, c):
        ref = piece(t, rep, c)
        return remote(ref, ref, z_s.at[j, c], z_r.at[t, c], (near_dev, across_dev)[j])

    def z_wait(k, c):
        ref = piece(srcs[k], rep, c)
        remote(ref, ref, z_s.at[0, c], z_r.at[srcs[k], c], near_dev).wait_recv()

    def z_relay(k, c):
        ref = piece(srcs[k], rep, c)
        return remote(ref, ref, zr_s.at[k - 1, c], z_r.at[srcs[k], c], near_dev)

    def relay_weights(k, c):
        @pl.when(inner)
        def _():
            z_wait(k, c)
            z_relay(k, c).start()

    def end_wait(k, c):
        @pl.when(jnp.logical_not(inner))
        def _():
            z_wait(k, c)

    def a_copy(k, c, j):
        ref = piece(srcs[k], rep, c)
        return remote(ref, ref, a_s.at[k, c, j], a_r.at[k, c, j], (x_peer, y_peer, partner)[j])

    def a_start(k, c, *ways):
        for j in ways:
            a_copy(k, c, j).start()

    def a_wait(k, c, j):
        ref = piece(srcs[k], (rep_x, rep_y)[j], c)
        remote(ref, ref, a_s.at[k, c, j], a_r.at[k, c, j], (x_peer, y_peer)[j]).wait_recv()

    def b_copy(k, c, j):
        r = (rep_x, rep_y, rep_x, rep_y)[j]
        ref = (piece(srcs[k], r, c), piece(srcs[k], r, c), piece(srcs[k], r, c, 0, cut), piece(srcs[k], r, c, cut, part_rows - cut))[j]
        return remote(ref, ref, b_s.at[k, c, j], b_r.at[k, c, j], (partner, partner, y_peer, x_peer)[j])

    def phase_b(k, c):
        a_wait(k, c, 1)
        b_copy(k, c, 3).start()
        b_copy(k, c, 1).start()
        a_wait(k, c, 0)
        b_copy(k, c, 2).start()
        b_copy(k, c, 0).start()

    def c_copy(k, c):
        ref = piece(srcs[k], rep_d, c)
        return remote(ref, ref, c_s.at[k, c], c_r.at[k, c], partner)

    def phase_c(k, c):
        for j, ref in ((2, piece(srcs[k], rep_d, c, 0, cut)), (3, piece(srcs[k], rep_d, c, cut, part_rows - cut))):
            remote(ref, ref, b_s.at[k, c, j], b_r.at[k, c, j], partner).wait_recv()
        c_copy(k, c).start()

    def weights_done():
        rp = s + 1 - 2 * core
        ry = (rp + 2) % 4
        base, base_x = b * n_seq, (1 - b) * n_seq
        for k in range(3):
            for c in range(2):
                for ref, ssem, rsem in (
                    (piece(srcs[k], base + rp, c), a_s.at[k, c, 2], a_r.at[k, c, 2]),
                    (piece(srcs[k], base_x + rp, c), b_s.at[k, c, 0], b_r.at[k, c, 0]),
                    (piece(srcs[k], base + ry, c), b_s.at[k, c, 1], b_r.at[k, c, 1]),
                    (piece(srcs[k], base_x + ry, c), c_s.at[k, c], c_r.at[k, c]),
                ):
                    remote(ref, ref, ssem, rsem, partner).wait_recv()

    for j in range(2):
        for c in range(2):
            z_copy(j, c).start()

    mine = pl.ds(pl.multiple_of(core * half, half), half)
    theirs = pl.ds(pl.multiple_of((1 - core) * half, half), half)

    def swap(ref, r1, s1, r2, full, ssem, rsem):
        first = remote(ref.at[theirs], r1, ssem.at[0], rsem.at[0], partner)
        second = remote(s1, r2, ssem.at[1], rsem.at[1], y_peer)
        third = remote(full.at[mine], full.at[mine], ssem.at[2], rsem.at[2], partner)
        third_in = remote(full.at[theirs], full.at[theirs], ssem.at[2], rsem.at[2], partner)
        return first, second, third, third_in

    qs1, qs2, qs3, qs3_in = swap(qsel_ref, qsel_r1, qsel_s1, qsel_r2, qsel_all, qsel_s, qsel_r)
    sel1, sel2, sel3, sel3_in = swap(sel_ref, sel_r1, sel_s1, sel_r2, sel_all, sel_s, sel_r)

    def pick_cols(i):
        cols = lax.broadcasted_iota(jnp.int32, (num_glob, BLK), 1) + i * BLK
        return jnp.where(slot_col[...] == cols, 1.0, 0.0).astype(BF16)

    acc_ref[...] = jnp.zeros_like(acc_ref)
    wload[2].wait()

    def project_g(i, carry):
        load_x(i).wait()
        at = pl.ds(pl.multiple_of(i * BLK, BLK), BLK)
        qg = dot_nn(x_ref[at, :], wg_ref[...]).astype(BF16) * scale
        acc_ref[:, 2 * width:] += dot_nn(pick_cols(i), qg)
        return carry

    lax.fori_loop(0, blocks, project_g, 0)
    qsel_ref[...] = acc_ref[:, 2 * width:].astype(BF16)
    qs1.start()
    wload[0].wait()
    wload[1].wait()

    def project(i, carry):
        at = pl.ds(pl.multiple_of(i * BLK, BLK), BLK)
        x = x_ref[at, :]
        k = dot_nn(x, wk_ref[...]).astype(BF16)
        v = dot_nn(x, wv_ref[...]).astype(BF16)
        ext = pl.ds(pl.multiple_of(i * BLK + window, BLK), BLK)
        kvx[ext, :width] = k
        kvx[ext, width:] = v
        pick = pick_cols(i)
        acc_ref[:, :width] += dot_nn(pick, k)
        acc_ref[:, width:2 * width] += dot_nn(pick, v)

        @pl.when(i == 1)
        def _():
            qs1.wait_recv()
            qsel_s1[...] = qsel_ref[mine, :] + qsel_r1[...]
            qs2.start()
            relay_weights(1, 0)
            z_wait(0, 0)
            a_start(0, 0, 0, 1, 2)

        @pl.when(i == 6)
        def _():
            qs2.wait_recv()
            qsel_all[mine, :] = qsel_s1[...] + qsel_r2[...]
            qs3.start()

        return carry

    lax.fori_loop(0, blocks, project, 0)
    sel_ref[...] = acc_ref[:, :2 * width].astype(BF16)
    sel1.start()
    halo_left = remote(kvx.at[pl.ds(window, window)], kvx.at[pl.ds(rows + window, window)], halo_s.at[0], halo_r.at[0], {"sp": (s + 3) % n_seq})
    halo_right = remote(kvx.at[pl.ds(rows, window)], kvx.at[pl.ds(0, window)], halo_s.at[1], halo_r.at[1], {"sp": (s + 1) % n_seq})
    has_left, has_right = s > 0, s < n_seq - 1
    relay_weights(1, 1)

    @pl.when(has_left)
    def _():
        halo_left.start()

    @pl.when(has_right)
    def _():
        halo_right.start()

    @pl.when(jnp.logical_not(has_left))
    def _():
        kvx[pl.ds(0, window), :] = jnp.zeros((window, 2 * width), BF16)

    @pl.when(jnp.logical_not(has_right))
    def _():
        kvx[pl.ds(rows + window, window), :] = jnp.zeros((window, 2 * width), BF16)

    z_wait(0, 1)
    a_start(0, 1, 0, 1, 2)
    qs3_in.wait_recv()

    lane_p = lax.broadcasted_iota(jnp.int32, (1, pair), 1)
    low = lane_p < head_dim
    zero = jnp.zeros((), BF16)
    tile = 128

    def masked(xv, odd):
        return jnp.where(low, zero, xv) if odd else jnp.where(low, xv, zero)

    def glob(i, carry):
        at = pl.ds(pl.multiple_of(i * tile, tile), tile)
        lane = lax.broadcasted_iota(jnp.int32, (tile, 128), 1)
        stat = jnp.zeros((tile, 128), F32)
        for p in range(heads // 2):
            qg = qsel_all[at, p * pair:(p + 1) * pair]
            k = kvx[pl.ds(window, rows), p * pair:(p + 1) * pair]
            v = kvx[pl.ds(window, rows), width + p * pair:width + (p + 1) * pair]
            outs = []
            for odd in (0, 1):
                sc = dot_nt(masked(qg, odd), k)
                m = jnp.max(sc, axis=1, keepdims=True)
                e = jnp.exp(sc - m)
                stat = jnp.where(lane == 2 * p + odd, m, stat)
                stat = jnp.where(lane == heads + 2 * p + odd, jnp.sum(e, axis=1, keepdims=True), stat)
                outs.append(dot_nn(e.astype(BF16), v))
            g_ref[at, p * pair:(p + 1) * pair] = jnp.where(low, outs[0], outs[1])
        g_ref[at, width:] = stat

        @pl.when(i == 0)
        def _():
            sel1.wait_recv()
            sel_s1[...] = sel_ref[mine, :] + sel_r1[...]
            sel2.start()

        @pl.when(i == 2)
        def _():
            end_wait(1, 0)
            a_start(1, 0, 0, 2)

        return carry

    lax.fori_loop(0, num_glob // tile, glob, 0)

    def merge(a, c):
        sa, sc = a[:, width:], c[:, width:]
        lane = lax.broadcasted_iota(jnp.int32, sa.shape, 1)
        wide = lax.broadcasted_iota(jnp.int32, (1, width), 1)
        fa = jnp.zeros((sa.shape[0], width), F32)
        fc, total = fa, fa
        stat = jnp.zeros_like(sa)
        for h in range(heads):
            ma, mc = sa[:, h:h + 1], sc[:, h:h + 1]
            la, lc = sa[:, heads + h:heads + h + 1], sc[:, heads + h:heads + h + 1]
            m = jnp.maximum(ma, mc)
            ea, ec = jnp.exp(ma - m), jnp.exp(mc - m)
            l = la * ea + lc * ec
            here = (wide >= h * head_dim) & (wide < (h + 1) * head_dim)
            fa = jnp.where(here, ea, fa)
            fc = jnp.where(here, ec, fc)
            total = jnp.where(here, l, total)
            stat = jnp.where(lane == h, m, stat)
            stat = jnp.where(lane == heads + h, l, stat)
        return a[:, :width] * fa + c[:, :width] * fc, total, stat

    g1, g2, g3, g3_in = swap(g_ref, g_r1, g_s1, g_r2, gout_ref, g_s, g_r)
    g1.start()
    sel2.wait_recv()
    sel_all[mine, :] = sel_s1[...] + sel_r2[...]
    sel3.start()

    wload[3].wait()

    def project_q(i, carry):
        at = pl.ds(pl.multiple_of(i * BLK, BLK), BLK)
        q_ref[at, :] = dot_nn(x_ref[at, :], wq_ref[...]).astype(BF16) * scale

        @pl.when(i == 2)
        def _():
            g1.wait_recv()
            num, total, stat = merge(g_ref[mine, :], g_r1[...])
            g_s1[:, :width] = num
            g_s1[:, width:] = stat
            g2.start()
            a_start(1, 0, 1)
            relay_weights(2, 0)
            phase_b(0, 0)

        return carry

    lax.fori_loop(0, blocks, project_q, 0)

    cols = lax.broadcasted_iota(jnp.int32, (BLK, band_w), 1)

    def make_band(lo, hi):
        for h in range(heads):
            row = jnp.broadcast_to(bias_ref[h], (BLK, span))
            band = pltpu.roll(row, 0, 1, stride=1, stride_axis=0)[:, :band_w]
            band_ref[h] = jnp.where((cols >= lo) & (cols < hi), band, -jnp.inf)

    is_first = 1 - (s + n_seq - 1) // n_seq
    is_last = s // (n_seq - 1)
    make_band(window * is_first, band_w)
    end_wait(1, 1)
    a_start(1, 1, 0, 1, 2)

    @pl.when(has_left)
    def _():
        halo_right.wait_recv()

    @pl.when(has_right)
    def _():
        halo_left.wait_recv()

    sel3_in.wait_recv()

    slot = slot_row[...]
    lane_b = lax.broadcasted_iota(jnp.int32, (BLK, pair), 1)
    row_iota = lax.broadcasted_iota(jnp.int32, (BLK, num_glob), 0)

    def attend(i):
        dist = slot - i * BLK - row_iota
        near_by = jnp.abs(dist) <= window
        start = pl.multiple_of(i * BLK, BLK)
        for p in range(heads // 2):
            at = slice(p * pair, (p + 1) * pair)
            q = q_ref[pl.ds(start, BLK), at]
            k_win = kvx[pl.ds(start, band_w), at]
            v_win = kvx[pl.ds(start, band_w), width + p * pair:width + (p + 1) * pair]
            k_glob = sel_all[:, p * pair:(p + 1) * pair]
            v_glob = sel_all[:, width + p * pair:width + (p + 1) * pair]
            outs = []
            for odd in (0, 1):
                qh = masked(q, odd)
                s_win = dot_nt(qh, k_win) + band_ref[2 * p + odd]
                s_glob = jnp.where(near_by, -jnp.inf, dot_nt(qh, k_glob))
                m = jnp.maximum(jnp.max(s_win, axis=1, keepdims=True), jnp.max(s_glob, axis=1, keepdims=True))
                e_win = jnp.exp(s_win - m)
                e_glob = jnp.exp(s_glob - m)
                inv = 1.0 / (jnp.sum(e_win, axis=1, keepdims=True) + jnp.sum(e_glob, axis=1, keepdims=True))
                o = dot_nn((e_win * inv).astype(BF16), v_win)
                outs.append(o + dot_nn((e_glob * inv).astype(BF16), v_glob))
            o_raw[pl.ds(start, BLK), at] = jnp.where(low, outs[0], outs[1]).astype(BF16)

    def block_ref(src, j):
        return o_all.at[src, pl.ds(pl.multiple_of(j * BLK, BLK), BLK)]

    def o_copy(j, way):
        return remote(block_ref(t, j), block_ref(t, j), o_s.at[way, j], o_r.at[t, j], (near_dev, across_dev)[way])

    def o_wait(src, j):
        remote(block_ref(src, j), block_ref(src, j), o_s.at[0, 0], o_r.at[src, j], near_dev).wait_recv()

    def o_relay(k, j):
        return remote(block_ref(srcs[k], j), block_ref(srcs[k], j), or_s.at[k - 1, j], o_r.at[srcs[k], j], near_dev)

    def finish(j, carry):
        at = pl.ds(pl.multiple_of(j * BLK, BLK), BLK)
        pick = jnp.where(slot - j * BLK == row_iota, 1.0, 0.0)
        is_glob = jnp.max(pick, axis=1, keepdims=True) > 0.0
        ins = dot_nn(pick.astype(BF16), gout_ref[...])
        o_all[t, at, :] = jnp.where(is_glob, ins, o_raw[at, :].astype(F32)).astype(BF16)
        o_copy(j, 0).start()
        o_copy(j, 1).start()
        return carry

    def relay(j, carry):
        for k in (1, 2):
            o_wait(srcs[k], j)
            o_relay(k, j).start()
        return carry

    def relays(lo, hi):
        @pl.when(inner)
        def _():
            lax.fori_loop(lo, hi, relay, 0)

    lag = 2

    def window_step(i, carry):
        attend(i)

        @pl.when(i == 0)
        def _():
            make_band(0, band_w)
            relay_weights(2, 1)
            phase_b(0, 1)

        @pl.when(i == 1)
        def _():
            g2.wait_recv()
            num, total, stat = merge(g_s1[...], g_r2[...])
            gout_ref[mine, :] = (num / total).astype(BF16)
            g3.start()

        @pl.when(i == 2)
        def _():
            phase_b(1, 0)

        @pl.when(i == 3)
        def _():
            end_wait(2, 0)
            a_start(2, 0, 0, 1, 2)
            phase_c(0, 0)

        @pl.when(i == 4)
        def _():
            phase_b(1, 1)

        @pl.when(i == 5)
        def _():
            end_wait(2, 1)
            a_start(2, 1, 0, 1, 2)
            phase_c(0, 1)

        @pl.when(i == 6)
        def _():
            make_band(0, band_w - window * is_last)

        @pl.when(i == 7)
        def _():
            phase_b(2, 0)
            phase_c(1, 0)

        @pl.when(i == lag)
        def _():
            g3_in.wait_recv()
            lax.fori_loop(0, lag, finish, 0)

        @pl.when(i >= lag)
        def _():
            finish(i, 0)

        @pl.when(i >= 4)
        def _():
            relays(i - 4, i - 3)

        return carry

    lax.fori_loop(0, blocks, window_step, 0)
    phase_c(1, 1)
    phase_b(2, 1)
    phase_c(2, 0)
    relays(4, 5)
    phase_c(2, 1)
    weights_done()

    def out_copy(i):
        return pltpu.make_async_copy(stage.at[i % 2], out_hbm.at[pl.ds(pl.multiple_of(i * BLK, BLK), BLK)], out_sem.at[i % 2])

    def mlp(i, carry):
        at = pl.ds(pl.multiple_of(i * BLK, BLK), BLK)
        o_wait(near, i)

        @pl.when(jnp.logical_not(inner))
        def _():
            o_wait(across, i)
            o_wait(far, i)

        acc = x_ref[at, :].astype(F32)
        for j in range(n_tp):
            acc += dot_nn(o_all[j, at, :], wbuf[j, :, 2 * up_rows:, :].reshape(width, dim))
        hidden = acc.astype(BF16)
        acc = hidden.astype(F32)
        for j in range(n_tp):
            up = dot_nn(hidden, wbuf[j, :, :up_rows, :].reshape(dim, dim))
            acc += dot_nn(jax.nn.gelu(up).astype(BF16), wbuf[j, :, up_rows:2 * up_rows, :].reshape(dim, dim))

        @pl.when(i >= 2)
        def _():
            out_copy(i - 2).wait()

        stage[i % 2] = acc.astype(BF16)
        out_copy(i).start()

        @pl.when(i == 0)
        def _():
            relays(5, 6)

        @pl.when(i == 1)
        def _():
            relays(6, 8)

        return carry

    lax.fori_loop(0, blocks, mlp, 0)

    out_copy(blocks - 2).wait()
    out_copy(blocks - 1).wait()
    @pl.when(has_left)
    def _():
        halo_left.wait_send()

    @pl.when(has_right)
    def _():
        halo_right.wait_send()

    for copy in (qs1, qs2, qs3, sel1, sel2, sel3, g1, g2, g3):
        copy.wait_send()
    for c in range(2):
        z_copy(0, c).wait_send()
        z_copy(1, c).wait_send()
        for k in range(3):
            for j in range(3):
                a_copy(k, c, j).wait_send()
            for j in range(4):
                b_copy(k, c, j).wait_send()
            c_copy(k, c).wait_send()

    def drain(j, carry):
        o_copy(j, 0).wait_send()
        o_copy(j, 1).wait_send()
        return carry

    lax.fori_loop(0, blocks, drain, 0)

    @pl.when(inner)
    def _():
        for k in (1, 2):
            for c in range(2):
                z_relay(k, c).wait_send()

        def drain_relay(j, carry):
            o_relay(1, j).wait_send()
            o_relay(2, j).wait_send()
            return carry

        lax.fori_loop(0, blocks, drain_relay, 0)


def solution(mesh):
    n_seq = mesh.shape["sp"]
    n_tp = mesh.shape["tp"]
    n_batch = mesh.shape["batch"]
    n_rep = n_seq * n_batch

    def local_layer(tokens, glob_pos, rel_bias, w_query, w_key, w_value, w_query_glob, w_out, w_up, w_down):
        rows, dim = tokens.shape
        heads = rel_bias.shape[0]
        window = (rel_bias.shape[1] - 1) // 2
        width = w_query.shape[1]
        head_dim = width // heads
        num_glob = glob_pos.shape[0]
        half = num_glob // 2
        slot = glob_pos - lax.axis_index("sp") * rows
        span = 4 * window
        bias = jnp.pad(rel_bias, ((0, 0), (0, span - rel_bias.shape[1])), constant_values=-jnp.inf)[:, None]
        blocks = rows // BLK
        up_rows, out_rows = dim // n_rep, width // n_rep
        stat_w = width + 128
        any_spec = pl.BlockSpec(memory_space=pl.ANY)
        vmem_spec = pl.BlockSpec(memory_space=pltpu.VMEM)
        dma = pltpu.SemaphoreType.DMA
        return pl.pallas_call(
            functools.partial(layer_kernel, n_tp, n_seq, window, head_dim, heads),
            out_shape=jax.ShapeDtypeStruct((rows, dim), BF16),
            in_specs=[vmem_spec] * 3 + [any_spec] * 8,
            out_specs=any_spec,
            scratch_shapes=[
                pltpu.VMEM((rows, dim), BF16),
                pltpu.VMEM((dim, width), BF16),
                pltpu.VMEM((dim, width), BF16),
                pltpu.VMEM((dim, width), BF16),
                pltpu.VMEM((dim, width), BF16),
                pltpu.VMEM((n_tp, n_rep, 2 * up_rows + out_rows, dim), BF16),
                pltpu.VMEM((rows, width), BF16),
                pltpu.VMEM((rows + 2 * window, 2 * width), BF16),
                pltpu.VMEM((num_glob, 3 * width), F32),
                *[pltpu.VMEM((n, width), BF16) for n in (num_glob, half, half, half, num_glob)],
                *[pltpu.VMEM((n, 2 * width), BF16) for n in (num_glob, half, half, half, num_glob)],
                pltpu.VMEM((heads, BLK, 3 * window), F32),
                pltpu.VMEM((num_glob, stat_w), F32),
                pltpu.VMEM((half, stat_w), F32),
                pltpu.VMEM((half, stat_w), F32),
                pltpu.VMEM((half, stat_w), F32),
                pltpu.VMEM((num_glob, width), BF16),
                pltpu.VMEM((rows, width), BF16),
                pltpu.VMEM((n_tp, rows, width), BF16),
                pltpu.VMEM((2, BLK, dim), BF16),
                dma((blocks,)), dma((4,)), dma((3,)), dma((2,)),
                dma((2,)), dma((2,)), *[dma((3,))] * 6,
                dma((2, 2)), dma((n_tp, 2)), dma((2, 2)),
                dma((3, 2, 3)), dma((3, 2, 3)), dma((3, 2, 4)), dma((3, 2, 4)), dma((3, 2)), dma((3, 2)),
                dma((2, blocks)), dma((n_tp, blocks)), dma((2, blocks)),
            ],
            compiler_params=pltpu.CompilerParams(vmem_limit_bytes=VMEM_CAP, collective_id=0, has_side_effects=True),
            name="layer",
        )(
            slot[:, None], slot[None], bias, tokens, w_query, w_key, w_value, w_query_glob,
            w_up.reshape(n_rep, up_rows, dim), w_down.reshape(n_rep, up_rows, dim), w_out.reshape(n_rep, out_rows, dim),
        )

    row_spec = P(("batch", "sp"), None)
    col_spec = P(None, "tp")
    head_spec = P("tp", None)
    in_specs = (row_spec, P("batch"), head_spec, col_spec, col_spec, col_spec, col_spec, head_spec, col_spec, head_spec)
    return jax.shard_map(local_layer, mesh=mesh, in_specs=in_specs, out_specs=row_spec, check_vma=False)
```

```python
import functools

import jax
import jax.numpy as jnp
from jax import lax
from jax.experimental import pallas as pl
from jax.experimental.pallas import tpu as pltpu
from jax.sharding import PartitionSpec as P

BLK = 256
F32 = jnp.float32
BF16 = jnp.bfloat16
MESH = pl.DeviceIdType.MESH
VMEM_CAP = 67043328


def dot_nn(a, b):
    return lax.dot_general(a, b, (((1,), (0,)), ((), ())), preferred_element_type=F32)


def dot_nt(a, b):
    return lax.dot_general(a, b, (((1,), (1,)), ((), ())), preferred_element_type=F32)


def layer_kernel(
    n_tp, n_seq, window, head_dim, heads,
    pos_ref, bias_ref, x_hbm, wq_hbm, wk_hbm, wv_hbm, wg_hbm, wu_hbm, wd_hbm, wo_hbm,
    out_hbm,
    x_ref, wq_ref, wk_ref, wv_ref, wg_ref, wbuf, q_ref, kvx, acc_ref, qsel_ref, qsel_r1, qsel_s1, qsel_r2, qsel_all, sel_ref, sel_r1, sel_s1, sel_r2, sel_all,
    band_ref, g_ref, g_r1, g_s1, g_r2, gout_ref, o_raw, o_all, stage,
    x_sem, w_sem, own_sem, out_sem, halo_s, halo_r, qsel_s, qsel_r, sel_s, sel_r, g_s, g_r,
    z_s, z_r, zr_s, a_s, a_r, b_s, b_r, c_s, c_r, o_s, o_r, or_s,
):
    rows, dim = x_ref.shape
    width = wq_ref.shape[1]
    num_glob = pos_ref.shape[1]
    half = num_glob // 2
    blocks = rows // BLK
    span = bias_ref.shape[1]
    band_w = 3 * window
    pair = 2 * head_dim
    scale = head_dim ** -0.5
    up_rows = wu_hbm.shape[1]
    out_rows = wo_hbm.shape[1]
    part_rows = (2 * up_rows + out_rows) // 2
    cut = part_rows // 3

    b = lax.axis_index("batch")
    t = lax.axis_index("tp")
    s = lax.axis_index("sp")
    core = s % 2
    partner = {"sp": s + 1 - 2 * core}
    y_peer = {"sp": (s + 2) % 4}
    x_peer = {"batch": 1 - b}
    near = t + 1 - 2 * (t % 2)
    side = t // 2
    across = 2 - side
    far = 3 - 3 * side
    inner = (t == 1) | (t == 2)
    near_dev, across_dev = {"tp": near}, {"tp": across}
    srcs = (near, across, far)
    rep = b * n_seq + s
    rep_x = (1 - b) * n_seq + s
    rep_y = b * n_seq + (s + 2) % 4
    rep_d = (1 - b) * n_seq + (s + 2) % 4

    def remote(src, dst, ssem, rsem, dev):
        return pltpu.make_async_remote_copy(src_ref=src, dst_ref=dst, send_sem=ssem, recv_sem=rsem, device_id=dev, device_id_type=MESH)

    def load_x(i):
        at = pl.ds(pl.multiple_of(i * BLK, BLK), BLK)
        return pltpu.make_async_copy(x_hbm.at[at], x_ref.at[at], x_sem.at[i])

    own = [
        pltpu.make_async_copy(wu_hbm, wbuf.at[t, :, pl.ds(0, up_rows)], own_sem.at[0]),
        pltpu.make_async_copy(wd_hbm, wbuf.at[t, :, pl.ds(up_rows, up_rows)], own_sem.at[1]),
        pltpu.make_async_copy(wo_hbm, wbuf.at[t, :, pl.ds(2 * up_rows, out_rows)], own_sem.at[2]),
    ]
    wload = [pltpu.make_async_copy(h, v, w_sem.at[j]) for j, (h, v) in enumerate(((wk_hbm, wk_ref), (wv_hbm, wv_ref), (wg_hbm, wg_ref), (wq_hbm, wq_ref)))]
    for copy in own:
        copy.start()
    for copy in wload:
        copy.start()
    for i in range(blocks):
        load_x(i).start()

    barrier = pltpu.get_barrier_semaphore()
    peers = [{"tp": (t + d) % n_tp} for d in (1, 2, 3)] + [{"sp": (s + d) % n_seq} for d in (1, 2, 3)] + [x_peer]
    for dev in peers:
        pl.semaphore_signal(barrier, inc=1, device_id=dev, device_id_type=MESH)
    pl.semaphore_wait(barrier, len(peers))
    for copy in own:
        copy.wait()

    def piece(src, r, c, lo=0, size=part_rows):
        return wbuf.at[src, r, pl.ds(c * part_rows + lo, size)]

    def z_copy(j, c):
        ref = piece(t, rep, c)
        return remote(ref, ref, z_s.at[j, c], z_r.at[t, c], (near_dev, across_dev)[j])

    def z_wait(k, c):
        ref = piece(srcs[k], rep, c)
        remote(ref, ref, z_s.at[0, c], z_r.at[srcs[k], c], near_dev).wait_recv()

    def z_relay(k, c):
        ref = piece(srcs[k], rep, c)
        return remote(ref, ref, zr_s.at[k - 1, c], z_r.at[srcs[k], c], near_dev)

    def relay_weights(k, c):
        @pl.when(inner)
        def _():
            z_wait(k, c)
            z_relay(k, c).start()

    def end_wait(k, c):
        @pl.when(jnp.logical_not(inner))
        def _():
            z_wait(k, c)

    def a_copy(k, c, j):
        ref = piece(srcs[k], rep, c)
        return remote(ref, ref, a_s.at[k, c, j], a_r.at[k, c, j], (x_peer, y_peer, partner)[j])

    def a_start(k, c, *ways):
        for j in ways:
            a_copy(k, c, j).start()

    def a_wait(k, c, j):
        ref = piece(srcs[k], (rep_x, rep_y)[j], c)
        remote(ref, ref, a_s.at[k, c, j], a_r.at[k, c, j], (x_peer, y_peer)[j]).wait_recv()

    def b_copy(k, c, j):
        r = (rep_x, rep_y, rep_x, rep_y)[j]
        ref = (piece(srcs[k], r, c), piece(srcs[k], r, c), piece(srcs[k], r, c, 0, cut), piece(srcs[k], r, c, cut, part_rows - cut))[j]
        return remote(ref, ref, b_s.at[k, c, j], b_r.at[k, c, j], (partner, partner, y_peer, x_peer)[j])

    def phase_b(k, c):
        a_wait(k, c, 1)
        b_copy(k, c, 3).start()
        b_copy(k, c, 1).start()
        a_wait(k, c, 0)
        b_copy(k, c, 2).start()
        b_copy(k, c, 0).start()

    def c_copy(k, c):
        ref = piece(srcs[k], rep_d, c)
        return remote(ref, ref, c_s.at[k, c], c_r.at[k, c], partner)

    def phase_c(k, c):
        for j, ref in ((2, piece(srcs[k], rep_d, c, 0, cut)), (3, piece(srcs[k], rep_d, c, cut, part_rows - cut))):
            remote(ref, ref, b_s.at[k, c, j], b_r.at[k, c, j], partner).wait_recv()
        c_copy(k, c).start()

    def weights_done():
        rp = s + 1 - 2 * core
        ry = (rp + 2) % 4
        base, base_x = b * n_seq, (1 - b) * n_seq
        for k in range(3):
            for c in range(2):
                for ref, ssem, rsem in (
                    (piece(srcs[k], base + rp, c), a_s.at[k, c, 2], a_r.at[k, c, 2]),
                    (piece(srcs[k], base_x + rp, c), b_s.at[k, c, 0], b_r.at[k, c, 0]),
                    (piece(srcs[k], base + ry, c), b_s.at[k, c, 1], b_r.at[k, c, 1]),
                    (piece(srcs[k], base_x + ry, c), c_s.at[k, c], c_r.at[k, c]),
                ):
                    remote(ref, ref, ssem, rsem, partner).wait_recv()

    for c in range(2):
        for j in range(2):
            z_copy(j, c).start()

    mine = pl.ds(pl.multiple_of(core * half, half), half)
    theirs = pl.ds(pl.multiple_of((1 - core) * half, half), half)

    def swap(ref, r1, s1, r2, full, ssem, rsem):
        first = remote(ref.at[theirs], r1, ssem.at[0], rsem.at[0], partner)
        second = remote(s1, r2, ssem.at[1], rsem.at[1], y_peer)
        third = remote(full.at[mine], full.at[mine], ssem.at[2], rsem.at[2], partner)
        third_in = remote(full.at[theirs], full.at[theirs], ssem.at[2], rsem.at[2], partner)
        return first, second, third, third_in

    qs1, qs2, qs3, qs3_in = swap(qsel_ref, qsel_r1, qsel_s1, qsel_r2, qsel_all, qsel_s, qsel_r)
    sel1, sel2, sel3, sel3_in = swap(sel_ref, sel_r1, sel_s1, sel_r2, sel_all, sel_s, sel_r)

    slot = pos_ref[...] - s * rows
    slot_col = jnp.transpose(jnp.broadcast_to(slot, (8, num_glob)))[:, :1]

    def pick_cols(i):
        cols = lax.broadcasted_iota(jnp.int32, (num_glob, BLK), 1) + i * BLK
        return jnp.where(slot_col == cols, 1.0, 0.0).astype(BF16)

    acc_ref[...] = jnp.zeros_like(acc_ref)
    wload[2].wait()

    def project_g(i, carry):
        load_x(i).wait()
        at = pl.ds(pl.multiple_of(i * BLK, BLK), BLK)
        qg = dot_nn(x_ref[at, :], wg_ref[...]).astype(BF16) * scale
        acc_ref[:, 2 * width:] += dot_nn(pick_cols(i), qg)
        return carry

    lax.fori_loop(0, blocks, project_g, 0)
    qsel_ref[...] = acc_ref[:, 2 * width:].astype(BF16)
    qs1.start()
    wload[0].wait()
    wload[1].wait()

    def project(i, carry):
        at = pl.ds(pl.multiple_of(i * BLK, BLK), BLK)
        x = x_ref[at, :]
        k = dot_nn(x, wk_ref[...]).astype(BF16)
        v = dot_nn(x, wv_ref[...]).astype(BF16)
        ext = pl.ds(pl.multiple_of(i * BLK + window, BLK), BLK)
        kvx[ext, :width] = k
        kvx[ext, width:] = v
        pick = pick_cols(i)
        acc_ref[:, :width] += dot_nn(pick, k)
        acc_ref[:, width:2 * width] += dot_nn(pick, v)

        @pl.when(i == 1)
        def _():
            qs1.wait_recv()
            qsel_s1[...] = qsel_ref[mine, :] + qsel_r1[...]
            qs2.start()
            relay_weights(1, 0)
            z_wait(0, 0)
            a_start(0, 0, 0, 1, 2)

        @pl.when(i == 6)
        def _():
            qs2.wait_recv()
            qsel_all[mine, :] = qsel_s1[...] + qsel_r2[...]
            qs3.start()

        return carry

    lax.fori_loop(0, blocks, project, 0)
    sel_ref[...] = acc_ref[:, :2 * width].astype(BF16)
    sel1.start()
    halo_left = remote(kvx.at[pl.ds(window, window)], kvx.at[pl.ds(rows + window, window)], halo_s.at[0], halo_r.at[0], {"sp": (s + 3) % n_seq})
    halo_right = remote(kvx.at[pl.ds(rows, window)], kvx.at[pl.ds(0, window)], halo_s.at[1], halo_r.at[1], {"sp": (s + 1) % n_seq})
    has_left, has_right = s > 0, s < n_seq - 1
    relay_weights(1, 1)

    @pl.when(has_left)
    def _():
        halo_left.start()

    @pl.when(has_right)
    def _():
        halo_right.start()

    @pl.when(jnp.logical_not(has_left))
    def _():
        kvx[pl.ds(0, window), :] = jnp.zeros((window, 2 * width), BF16)

    @pl.when(jnp.logical_not(has_right))
    def _():
        kvx[pl.ds(rows + window, window), :] = jnp.zeros((window, 2 * width), BF16)

    z_wait(0, 1)
    a_start(0, 1, 0, 1, 2)
    qs3_in.wait_recv()

    lane_p = lax.broadcasted_iota(jnp.int32, (1, pair), 1)
    low = lane_p < head_dim
    zero = jnp.zeros((), BF16)
    tile = 128

    def masked(xv, odd):
        return jnp.where(low, zero, xv) if odd else jnp.where(low, xv, zero)

    def glob(i, carry):
        at = pl.ds(pl.multiple_of(i * tile, tile), tile)
        lane = lax.broadcasted_iota(jnp.int32, (tile, 128), 1)
        stat = jnp.zeros((tile, 128), F32)
        for p in range(heads // 2):
            qg = qsel_all[at, p * pair:(p + 1) * pair]
            k = kvx[pl.ds(window, rows), p * pair:(p + 1) * pair]
            v = kvx[pl.ds(window, rows), width + p * pair:width + (p + 1) * pair]
            outs = []
            for odd in (0, 1):
                sc = dot_nt(masked(qg, odd), k)
                m = jnp.max(sc, axis=1, keepdims=True)
                e = jnp.exp(sc - m)
                stat = jnp.where(lane == 2 * p + odd, m, stat)
                stat = jnp.where(lane == heads + 2 * p + odd, jnp.sum(e, axis=1, keepdims=True), stat)
                outs.append(dot_nn(e.astype(BF16), v))
            g_ref[at, p * pair:(p + 1) * pair] = jnp.where(low, outs[0], outs[1])
        g_ref[at, width:] = stat

        @pl.when(i == 0)
        def _():
            sel1.wait_recv()
            sel_s1[...] = sel_ref[mine, :] + sel_r1[...]
            sel2.start()

        @pl.when(i == 2)
        def _():
            end_wait(1, 0)
            a_start(1, 0, 0, 2)

        return carry

    lax.fori_loop(0, num_glob // tile, glob, 0)

    def merge(a, c):
        sa, sc = a[:, width:], c[:, width:]
        lane = lax.broadcasted_iota(jnp.int32, sa.shape, 1)
        wide = lax.broadcasted_iota(jnp.int32, (1, width), 1)
        fa = jnp.zeros((sa.shape[0], width), F32)
        fc, total = fa, fa
        stat = jnp.zeros_like(sa)
        for h in range(heads):
            ma, mc = sa[:, h:h + 1], sc[:, h:h + 1]
            la, lc = sa[:, heads + h:heads + h + 1], sc[:, heads + h:heads + h + 1]
            m = jnp.maximum(ma, mc)
            ea, ec = jnp.exp(ma - m), jnp.exp(mc - m)
            l = la * ea + lc * ec
            here = (wide >= h * head_dim) & (wide < (h + 1) * head_dim)
            fa = jnp.where(here, ea, fa)
            fc = jnp.where(here, ec, fc)
            total = jnp.where(here, l, total)
            stat = jnp.where(lane == h, m, stat)
            stat = jnp.where(lane == heads + h, l, stat)
        return a[:, :width] * fa + c[:, :width] * fc, total, stat

    g1, g2, g3, g3_in = swap(g_ref, g_r1, g_s1, g_r2, gout_ref, g_s, g_r)
    g1.start()
    sel2.wait_recv()
    sel_all[mine, :] = sel_s1[...] + sel_r2[...]
    sel3.start()

    wload[3].wait()

    def project_q(i, carry):
        at = pl.ds(pl.multiple_of(i * BLK, BLK), BLK)
        q_ref[at, :] = dot_nn(x_ref[at, :], wq_ref[...]).astype(BF16) * scale

        @pl.when(i == 2)
        def _():
            g1.wait_recv()
            num, total, stat = merge(g_ref[mine, :], g_r1[...])
            g_s1[:, :width] = num
            g_s1[:, width:] = stat
            g2.start()
            a_start(1, 0, 1)
            relay_weights(2, 0)
            phase_b(0, 0)

        return carry

    lax.fori_loop(0, blocks, project_q, 0)

    cols = lax.broadcasted_iota(jnp.int32, (BLK, band_w), 1)

    def make_band(lo, hi):
        for h in range(heads):
            row = jnp.broadcast_to(bias_ref[h:h + 1, :], (BLK, span))
            band = pltpu.roll(row, 0, 1, stride=1, stride_axis=0)[:, :band_w]
            band_ref[h] = jnp.where((cols >= lo) & (cols < hi), band, -jnp.inf)

    is_first = 1 - (s + n_seq - 1) // n_seq
    is_last = s // (n_seq - 1)
    make_band(window * is_first, band_w)
    end_wait(1, 1)
    a_start(1, 1, 0, 1, 2)

    @pl.when(has_left)
    def _():
        halo_right.wait_recv()

    @pl.when(has_right)
    def _():
        halo_left.wait_recv()

    sel3_in.wait_recv()

    lane_b = lax.broadcasted_iota(jnp.int32, (BLK, pair), 1)
    row_iota = lax.broadcasted_iota(jnp.int32, (BLK, num_glob), 0)

    def attend(i):
        dist = slot - i * BLK - row_iota
        near_by = jnp.abs(dist) <= window
        start = pl.multiple_of(i * BLK, BLK)
        for p in range(heads // 2):
            at = slice(p * pair, (p + 1) * pair)
            q = q_ref[pl.ds(start, BLK), at]
            k_win = kvx[pl.ds(start, band_w), at]
            v_win = kvx[pl.ds(start, band_w), width + p * pair:width + (p + 1) * pair]
            k_glob = sel_all[:, p * pair:(p + 1) * pair]
            v_glob = sel_all[:, width + p * pair:width + (p + 1) * pair]
            outs = []
            for odd in (0, 1):
                qh = masked(q, odd)
                s_win = dot_nt(qh, k_win) + band_ref[2 * p + odd]
                s_glob = jnp.where(near_by, -jnp.inf, dot_nt(qh, k_glob))
                m = jnp.maximum(jnp.max(s_win, axis=1, keepdims=True), jnp.max(s_glob, axis=1, keepdims=True))
                e_win = jnp.exp(s_win - m)
                e_glob = jnp.exp(s_glob - m)
                inv = 1.0 / (jnp.sum(e_win, axis=1, keepdims=True) + jnp.sum(e_glob, axis=1, keepdims=True))
                o = dot_nn((e_win * inv).astype(BF16), v_win)
                outs.append(o + dot_nn((e_glob * inv).astype(BF16), v_glob))
            o_raw[pl.ds(start, BLK), at] = jnp.where(low, outs[0], outs[1]).astype(BF16)

    def block_ref(src, j):
        return o_all.at[src, pl.ds(pl.multiple_of(j * BLK, BLK), BLK)]

    def o_copy(j, way):
        return remote(block_ref(t, j), block_ref(t, j), o_s.at[way, j], o_r.at[t, j], (near_dev, across_dev)[way])

    def o_wait(src, j):
        remote(block_ref(src, j), block_ref(src, j), o_s.at[0, 0], o_r.at[src, j], near_dev).wait_recv()

    def o_relay(k, j):
        return remote(block_ref(srcs[k], j), block_ref(srcs[k], j), or_s.at[k - 1, j], o_r.at[srcs[k], j], near_dev)

    def finish(j, carry):
        at = pl.ds(pl.multiple_of(j * BLK, BLK), BLK)
        pick = jnp.where(slot - j * BLK == row_iota, 1.0, 0.0)
        is_glob = jnp.max(pick, axis=1, keepdims=True) > 0.0
        ins = dot_nn(pick.astype(BF16), gout_ref[...])
        o_all[t, at, :] = jnp.where(is_glob, ins, o_raw[at, :].astype(F32)).astype(BF16)
        o_copy(j, 0).start()
        o_copy(j, 1).start()
        return carry

    def relay(j, carry):
        for k in (1, 2):
            o_wait(srcs[k], j)
            o_relay(k, j).start()
        return carry

    def relays(lo, hi):
        @pl.when(inner)
        def _():
            lax.fori_loop(lo, hi, relay, 0)

    lag = 2

    def window_step(i, carry):
        attend(i)

        @pl.when(i == 0)
        def _():
            make_band(0, band_w)
            relay_weights(2, 1)
            phase_b(0, 1)

        @pl.when(i == 1)
        def _():
            g2.wait_recv()
            num, total, stat = merge(g_s1[...], g_r2[...])
            gout_ref[mine, :] = (num / total).astype(BF16)
            g3.start()

        @pl.when(i == 2)
        def _():
            phase_b(1, 0)

        @pl.when(i == 3)
        def _():
            end_wait(2, 0)
            a_start(2, 0, 0, 1, 2)
            phase_c(0, 0)

        @pl.when(i == 4)
        def _():
            phase_b(1, 1)

        @pl.when(i == 5)
        def _():
            end_wait(2, 1)
            a_start(2, 1, 0, 1, 2)
            phase_c(0, 1)

        @pl.when(i == 6)
        def _():
            make_band(0, band_w - window * is_last)

        @pl.when(i == 7)
        def _():
            phase_b(2, 0)
            phase_c(1, 0)

        @pl.when(i == lag)
        def _():
            g3_in.wait_recv()
            lax.fori_loop(0, lag, finish, 0)

        @pl.when(i >= lag)
        def _():
            finish(i, 0)

        @pl.when(i >= 6)
        def _():
            relays(i - 6, i - 5)

        return carry

    lax.fori_loop(0, blocks, window_step, 0)
    phase_c(1, 1)
    phase_b(2, 1)
    phase_c(2, 0)
    phase_c(2, 1)
    relays(2, 4)
    weights_done()

    def out_copy(i):
        return pltpu.make_async_copy(stage.at[i % 2], out_hbm.at[pl.ds(pl.multiple_of(i * BLK, BLK), BLK)], out_sem.at[i % 2])

    def mlp(i, carry):
        at = pl.ds(pl.multiple_of(i * BLK, BLK), BLK)
        o_wait(near, i)

        @pl.when(jnp.logical_not(inner))
        def _():
            o_wait(across, i)
            o_wait(far, i)

        acc = x_ref[at, :].astype(F32)
        for j in range(n_tp):
            acc += dot_nn(o_all[j, at, :], wbuf[j, :, 2 * up_rows:, :].reshape(width, dim))
        hidden = acc.astype(BF16)
        acc = hidden.astype(F32)
        for j in range(n_tp):
            up = dot_nn(hidden, wbuf[j, :, :up_rows, :].reshape(dim, dim))
            acc += dot_nn(jax.nn.gelu(up).astype(BF16), wbuf[j, :, up_rows:2 * up_rows, :].reshape(dim, dim))

        @pl.when(i >= 2)
        def _():
            out_copy(i - 2).wait()

        stage[i % 2] = acc.astype(BF16)
        out_copy(i).start()

        @pl.when(i == 0)
        def _():
            relays(4, 6)

        @pl.when(i == 1)
        def _():
            relays(6, 8)

        return carry

    lax.fori_loop(0, blocks, mlp, 0)

    out_copy(blocks - 2).wait()
    out_copy(blocks - 1).wait()
    @pl.when(has_left)
    def _():
        halo_left.wait_send()

    @pl.when(has_right)
    def _():
        halo_right.wait_send()

    for copy in (qs1, qs2, qs3, sel1, sel2, sel3, g1, g2, g3):
        copy.wait_send()
    for c in range(2):
        z_copy(0, c).wait_send()
        z_copy(1, c).wait_send()
        for k in range(3):
            for j in range(3):
                a_copy(k, c, j).wait_send()
            for j in range(4):
                b_copy(k, c, j).wait_send()
            c_copy(k, c).wait_send()

    def drain(j, carry):
        o_copy(j, 0).wait_send()
        o_copy(j, 1).wait_send()
        return carry

    lax.fori_loop(0, blocks, drain, 0)

    @pl.when(inner)
    def _():
        for k in (1, 2):
            for c in range(2):
                z_relay(k, c).wait_send()

        def drain_relay(j, carry):
            o_relay(1, j).wait_send()
            o_relay(2, j).wait_send()
            return carry

        lax.fori_loop(0, blocks, drain_relay, 0)


def solution(mesh):
    n_seq = mesh.shape["sp"]
    n_tp = mesh.shape["tp"]
    n_batch = mesh.shape["batch"]
    n_rep = n_seq * n_batch

    def local_layer(tokens, glob_pos, rel_bias, w_query, w_key, w_value, w_query_glob, w_out, w_up, w_down):
        rows, dim = tokens.shape
        heads = rel_bias.shape[0]
        window = (rel_bias.shape[1] - 1) // 2
        width = w_query.shape[1]
        head_dim = width // heads
        num_glob = glob_pos.shape[0]
        half = num_glob // 2
        span = 4 * window
        bias = jnp.pad(rel_bias, ((0, 0), (0, span - rel_bias.shape[1])), constant_values=-jnp.inf)
        blocks = rows // BLK
        up_rows, out_rows = dim // n_rep, width // n_rep
        stat_w = width + 128
        any_spec = pl.BlockSpec(memory_space=pl.ANY)
        vmem_spec = pl.BlockSpec(memory_space=pltpu.VMEM)
        dma = pltpu.SemaphoreType.DMA
        return pl.pallas_call(
            functools.partial(layer_kernel, n_tp, n_seq, window, head_dim, heads),
            out_shape=jax.ShapeDtypeStruct((rows, dim), BF16),
            in_specs=[vmem_spec] * 2 + [any_spec] * 8,
            out_specs=any_spec,
            scratch_shapes=[
                pltpu.VMEM((rows, dim), BF16),
                pltpu.VMEM((dim, width), BF16),
                pltpu.VMEM((dim, width), BF16),
                pltpu.VMEM((dim, width), BF16),
                pltpu.VMEM((dim, width), BF16),
                pltpu.VMEM((n_tp, n_rep, 2 * up_rows + out_rows, dim), BF16),
                pltpu.VMEM((rows, width), BF16),
                pltpu.VMEM((rows + 2 * window, 2 * width), BF16),
                pltpu.VMEM((num_glob, 3 * width), F32),
                *[pltpu.VMEM((n, width), BF16) for n in (num_glob, half, half, half, num_glob)],
                *[pltpu.VMEM((n, 2 * width), BF16) for n in (num_glob, half, half, half, num_glob)],
                pltpu.VMEM((heads, BLK, 3 * window), F32),
                pltpu.VMEM((num_glob, stat_w), F32),
                pltpu.VMEM((half, stat_w), F32),
                pltpu.VMEM((half, stat_w), F32),
                pltpu.VMEM((half, stat_w), F32),
                pltpu.VMEM((num_glob, width), BF16),
                pltpu.VMEM((rows, width), BF16),
                pltpu.VMEM((n_tp, rows, width), BF16),
                pltpu.VMEM((2, BLK, dim), BF16),
                dma((blocks,)), dma((4,)), dma((3,)), dma((2,)),
                dma((2,)), dma((2,)), *[dma((3,))] * 6,
                dma((2, 2)), dma((n_tp, 2)), dma((2, 2)),
                dma((3, 2, 3)), dma((3, 2, 3)), dma((3, 2, 4)), dma((3, 2, 4)), dma((3, 2)), dma((3, 2)),
                dma((2, blocks)), dma((n_tp, blocks)), dma((2, blocks)),
            ],
            compiler_params=pltpu.CompilerParams(vmem_limit_bytes=VMEM_CAP, collective_id=0, has_side_effects=True),
            name="layer",
        )(
            glob_pos[None], bias, tokens, w_query, w_key, w_value, w_query_glob,
            w_up.reshape(n_rep, up_rows, dim), w_down.reshape(n_rep, up_rows, dim), w_out.reshape(n_rep, out_rows, dim),
        )

    row_spec = P(("batch", "sp"), None)
    col_spec = P(None, "tp")
    head_spec = P("tp", None)
    in_specs = (row_spec, P("batch"), head_spec, col_spec, col_spec, col_spec, col_spec, head_spec, col_spec, head_spec)
    return jax.shard_map(local_layer, mesh=mesh, in_specs=in_specs, out_specs=row_spec, check_vma=False)
```
